32 devices in a mesh: section: 8 (over z, y), dp: 4 (over x, core).
Axes of the slice: x: 2, y: 2, z: 4, core: 2. Of those that a mesh axis runs over, the one named last changes fastest.
Arguments:
- vit_weight: bfloat16 [8, 1280, 1280], P('section', 'dp'), may hold values from -0.078125 to 0.078125
- t5_weight: bfloat16 [8, 2048, 2048], P('section', 'dp'), may hold values from -0.0625 to 0.0625
- vit_saved: bfloat16 [8, 4, 128, 1280], P('section', None, 'dp'), may hold values from -6 to 6
- t5_saved: bfloat16 [8, 4, 128, 2048], P('section', None, 'dp'), may hold values from -6 to 6
- vit_top_grad: bfloat16 [4, 128, 1280], P(None, 'dp'), may hold values from -6 to 6
- t5_top_grad: bfloat16 [4, 128, 2048], P(None, 'dp'), may hold values from -6 to 6
Outputs:
- vit_input_grads: bfloat16 [8, 4, 128, 1280], P('section', None, 'dp')
- t5_input_grads: bfloat16 [8, 4, 128, 2048], P('section', None, 'dp')
- vit_weight_grads: float32 [8, 1280, 1280], P('section', 'dp')
- t5_weight_grads: float32 [8, 2048, 2048], P('section', 'dp')
The draws below stay inside these ranges and needn't reach their ends.
All inputs are finite; a program needn't handle non-finite values.
Results may differ from the reference program's by a relative error of at most 0.02.
Values may be sent and summed in bfloat16 or wider, within the bound.
A program may use at most 128 MiB of HBM per device.

```python
import jax
import jax.numpy as jnp
from jax import lax

DV = 1280
DT = 2048
TOK = 32
MB = 4
LAYERS = 8
TOKENS = 128
N_DP = 4


def spiked(entries, own_key, source, target, blocks, factor):
    owner, partner = [(jnp.arange(entries.shape[axis_at]) // (entries.shape[axis_at] // blocks)).reshape([-1 if axis == axis_at else 1 for axis in range(entries.ndim)]) for axis_at in (source, target)]
    chosen = jax.random.permutation(own_key, blocks)[partner]
    strong = (owner == chosen) | (owner == (partner + blocks // 2) % blocks)
    return jnp.where(strong, factor * entries, entries)


def level_of(own_key, shape, pieces, low, high):
    def one(dim, blocks):
        heights = jax.random.uniform(jax.random.fold_in(jax.random.fold_in(own_key, 6), dim), (blocks,), jnp.float32, low / len(pieces), high / len(pieces))
        return jnp.repeat(jnp.exp(heights), shape[dim] // blocks).reshape((-1,) + (1,) * (len(shape) - dim - 1))

    loudness = one(*pieces[0])
    for cut in pieces[1:]:
        loudness = loudness * one(*cut)
    return loudness


def normal_values(rng, shape, width, most, split=(), kind=jnp.bfloat16):
    drawn = jax.random.normal(rng, shape, jnp.float32) * width
    if len(split) > 0:
        drawn = level_of(rng, shape, split, -0.22, 0.18) * drawn
    return jnp.clip(drawn, min=-most, max=most).astype(kind)


def gaussian_with(own_key, dims, scale, bound, split, heavy, dtype=jnp.bfloat16):
    values = scale * jax.random.normal(own_key, dims, jnp.float32)
    if split:
        values = values * level_of(own_key, dims, split, -0.22, 0.18)
    return jnp.clip(spiked(values, jax.random.fold_in(own_key, 3), *heavy), -bound, bound).astype(dtype)


def setup_inputs(seed: int = 0) -> dict:
    keys = jax.random.split(jax.random.key(seed), 7)
    return {
        "vit_weight": normal_values(keys[0], (LAYERS, DV, DV), (4 * DV) ** -0.5, 0.078125, ((0, 8), (1, 4))),
        "t5_weight": normal_values(keys[1], (LAYERS, DT, DT), (4 * DT) ** -0.5, 0.0625, ((0, 8), (1, 4))),
        "vit_saved": gaussian_with(keys[2], (LAYERS, MB, TOKENS, DV), 1.0, 6.0, ((0, 8), (2, 4)), (2, 3, 4, 2.0)),
        "t5_saved": gaussian_with(keys[3], (LAYERS, MB, TOKENS, DT), 1.0, 6.0, ((0, 8), (2, 4)), (2, 3, 4, 2.0)),
        "vit_top_grad": normal_values(keys[4], (MB, TOKENS, DV), 1.0, 6.0, ((1, 4),)),
        "t5_top_grad": normal_values(keys[5], (MB, TOKENS, DT), 1.0, 6.0, ((1, 4),)),
    }


root_half = 0.7071067811865476
inv_root_tau = 0.3989422804014327


def gelu_slope(preact):
    cumulative = 0.5 * (1.0 + lax.erf(preact * root_half))
    density = jnp.exp(-0.5 * preact * preact) * inv_root_tau
    return cumulative + preact * density


def layer_back(grad_above, saved_input, weight):
    preact = jnp.dot(saved_input, weight, preferred_element_type=jnp.float32)
    upper = grad_above.astype(jnp.float32)
    local_grad = (upper * gelu_slope(preact)).astype(jnp.bfloat16)
    through = jnp.dot(local_grad, weight.T, preferred_element_type=jnp.float32)
    return (upper + through).astype(jnp.bfloat16), local_grad


def run_branch(weights, saved, top_grad):
    layer_count = weights.shape[0]
    features = top_grad.shape[2]
    grad_above = top_grad.reshape(MB * TOKENS, features)
    input_grads = [None] * layer_count
    weight_grads = [None] * layer_count
    for layer_index in reversed(range(layer_count)):
        saved_input = saved[layer_index].reshape(MB * TOKENS, features)
        grad_below, local_grad = layer_back(grad_above, saved_input, weights[layer_index])
        grouped_input = saved_input.astype(jnp.float32).reshape(MB, N_DP, TOK, features)
        grouped_local = local_grad.astype(jnp.float32).reshape(MB, N_DP, TOK, features)
        partial_value = jnp.einsum("mpti,mptj->pij", grouped_input, grouped_local) * (1.0 / (MB * TOK))
        rounded = lax.optimization_barrier(partial_value.astype(jnp.bfloat16))
        weight_grads[layer_index] = jnp.sum(rounded.astype(jnp.float32), axis=0)
        input_grads[layer_index] = grad_below.reshape(MB, TOKENS, features)
        grad_above = grad_below
    return jnp.stack(input_grads), jnp.stack(weight_grads)


def reference(vit_weight, t5_weight, vit_saved, t5_saved, vit_top_grad, t5_top_grad):
    vit_grads, vit_wgrads = run_branch(vit_weight, vit_saved, vit_top_grad)
    t5_grads, t5_wgrads = run_branch(t5_weight, t5_saved, t5_top_grad)
    return (vit_grads, t5_grads, vit_wgrads, t5_wgrads)
```

```python
import functools

import jax
import jax.numpy as jnp
from jax import lax
from jax.experimental import pallas as pl
from jax.experimental.pallas import tpu as pltpu
from jax.sharding import PartitionSpec as P

root_half = 0.7071067811865476
inv_root_tau = 0.3989422804014327
MESH = pl.DeviceIdType.MESH


def gelu_slope(preact):
    cumulative = 0.5 * (1.0 + lax.erf(preact * root_half))
    density = jnp.exp(-0.5 * preact * preact) * inv_root_tau
    return cumulative + preact * density


NAMES = (
    "saved", "top", "lifted", "columns", "local", "weight", "flip", "above", "below", "mine",
    "pair_out", "pair_in", "chip_in", "slopes", "sums", "saved_got", "above_got", "pair_got",
    "chip_got", "near_got", "far_got", "slope_got", "out_got", "sent", "top_sent", "top_got",
    "lift_sent",
)
SENDS = ("saved", "pair", "chip", "near", "far", "slope", "hop", "out", "columns", "local", "sums")


class Branch:
    def __init__(self, ins, outs, scratch):
        self.weight_in, self.saved_in, self.top_in = ins
        self.out, self.columns_out, self.local_out, self.sums_out = outs
        for name, ref in zip(NAMES, scratch):
            setattr(self, name, ref)


def drain(ref, sem):
    pltpu.make_async_copy(ref, ref, sem).wait()


def kernel(sections, parts, size, roomy, scale, *refs):
    ins, outs, scratch = refs[:6], refs[6:14], refs[14:]
    branches = [
        Branch(ins[3 * b : 3 * b + 3], outs[4 * b : 4 * b + 4],
               scratch[len(NAMES) * b : len(NAMES) * (b + 1)])
        for b in range(2)
    ]
    count = size * parts
    first_size = size // 2 if size % 2 == 0 else size
    section = lax.axis_index("section")
    me = lax.axis_index("dp")
    chips = parts // 2
    chip, core = me // 2, me % 2
    partner = chip * 2 + 1 - core
    last = sections - 1
    is_last = section == last
    is_first = section == 0
    wide_count = sections // 2 + 1 if roomy else 0
    wide_flag = lax.min(lax.max(wide_count - section, 0), 1)
    wide_in = section < wide_count
    wide_out = jnp.logical_and(section > 0, section <= wide_count)
    lag = lax.min(1 + (2 - 1) * lax.max(section - last + 1, 0), count)
    narrow_sums = lax.min(3 + 4 * (last - section) * (last - section), count)
    first_sums = narrow_sums + (min(4, count) - narrow_sums) * wide_flag

    def slot(part):
        return part if roomy else 0

    def ahead(k):
        return lax.rem(chip + k, chips) * 2 + core

    def behind(k):
        return lax.rem(chip + chips - k, chips) * 2 + core

    def other(group):
        return group + 1 - 2 * core

    def owner(m):
        turn = m // size
        return lax.rem(turn, chips) * 2 + 1 - turn // chips

    def copy(src, dst, sent, got, where, part):
        return pltpu.make_async_remote_copy(
            src_ref=src, dst_ref=dst, send_sem=sent, recv_sem=got,
            device_id=(where, part), device_id_type=MESH,
        )

    def sent(br, name):
        return br.sent.at[SENDS.index(name)]

    def padded(block, wide):
        spare = wide - block.shape[-1]
        if spare:
            block = jnp.concatenate([block, jnp.zeros((*block.shape[:-1], spare), block.dtype)], axis=-1)
        return block

    def regroup(source, groups):
        cut = source.shape[-1] // parts
        for group in range(parts):
            groups[group] = padded(source[..., group * cut : (group + 1) * cut], groups.shape[-1])

    barrier = pltpu.get_barrier_semaphore()
    for k in range(1, parts):
        pl.semaphore_signal(barrier, inc=1, device_id=(section, lax.rem(me + k, parts)), device_id_type=MESH)

    def greet(other_section):
        for part in range(parts):
            pl.semaphore_signal(barrier, inc=1, device_id=(other_section, part), device_id_type=MESH)

    @pl.when(is_last)
    def _():
        @pl.loop(0, last)
        def _(lower):
            pl.semaphore_signal(barrier, inc=1, device_id=(lower, me), device_id_type=MESH)

    @pl.when(jnp.logical_not(is_last))
    def _():
        greet(section + 1)

    with jax.named_scope("regroup_saved"):
        for br in branches:
            regroup(br.saved_in, br.saved)
            regroup(br.top_in, br.top)
    greeted = parts * lax.min(section, 1) + lax.min(last - section, 1)
    with jax.named_scope("barrier"):
        pl.semaphore_wait(barrier, parts - 1 + greeted)

    def helper(m):
        return last - lax.rem(m, sections)

    def saved_copy(br, turn, k):
        to = lax.rem(me + k, parts)
        return copy(br.saved.at[to], br.columns.at[turn], sent(br, "saved"), br.saved_got.at[turn], section, to)

    def top_copy(br, m, k):
        to, turn = lax.rem(me + k, parts), m // sections
        return copy(br.top.at[to, lax.rem(m, size)], br.lifted.at[turn], br.top_sent.at[turn], br.top_got.at[turn], section, to)

    def lift_copy(br, m):
        turn = m // sections
        return copy(br.lifted.at[turn], br.above.at[m, slot(me)], br.lift_sent.at[turn], br.above_got.at[m], last, me)

    def pair_copy(br, m):
        return copy(br.pair_out.at[m], br.pair_in.at[m], sent(br, "pair"), br.pair_got.at[m], section, partner)

    def chip_copy(br, m, k):
        return copy(br.mine.at[m, k], br.chip_in.at[m, k - 1], sent(br, "chip"), br.chip_got.at[m], section, ahead(k))

    def near_copy(br, m, k):
        group = behind(k)
        return copy(br.local.at[m, group], br.local.at[m, group], sent(br, "near"), br.near_got.at[m], section, partner)

    def far_copy(br, m, k):
        return copy(br.local.at[m, me], br.local.at[m, me], sent(br, "far"), br.far_got.at[m], section, ahead(k))

    def hop_copy(br, m, k):
        return copy(br.below.at[m], br.above.at[m, slot(me)], sent(br, "hop"), br.above_got.at[m], lax.max(section - 1, 0), ahead(k))

    def share_copy(br, m, k):
        group = behind(k)
        return copy(br.above.at[m, group], br.above.at[m, group], sent(br, "near"), br.near_got.at[m], section, partner)

    def slope_far(br, m, k):
        return copy(br.slopes.at[m, me], br.slopes.at[m, me], sent(br, "far"), br.far_got.at[m], section, ahead(k))

    def slope_near(br, m, k):
        group = behind(k)
        return copy(br.slopes.at[m, group], br.slopes.at[m, group], sent(br, "slope"), br.slope_got.at[m], section, partner)

    def out_copy(br, m):
        return copy(br.below.at[m], br.out.at[me, lax.rem(m, size)], sent(br, "out"), br.out_got.at[0], section, owner(m))

    def half_copy(br, h, k):
        to, span = lax.rem(me + k, parts), pl.ds(h * first_size, first_size)
        return copy(br.saved.at[to, span], br.columns.at[0, span], sent(br, "saved"), br.saved_got.at[h * parts], section, to)

    def piecewise(turn):
        return jnp.logical_and(is_last, turn == chips)

    def piece_copy(br, m, k):
        to, turn, at = lax.rem(me + k, parts), m // size, lax.rem(m, size)
        return copy(br.saved.at[to, at], br.columns.at[turn, at], sent(br, "saved"), br.saved_got.at[turn], section, to)

    def send_piece(m):
        @pl.when(jnp.logical_and(piecewise(m // size), owner(m) == me))
        def _():
            for br in branches:
                for k in range(1, parts):
                    piece_copy(br, m, k).start()

    def send_saved(first, end):
        @pl.loop(first, end)
        def _(turn):
            @pl.when(owner(turn * size) == me)
            def _():
                for br in branches:
                    br.columns[turn] = br.saved[me]

                @pl.when(turn == 0)
                def _():
                    @pl.loop(0, size // first_size)
                    def _(h):
                        for br in branches:
                            for k in range(1, parts):
                                half_copy(br, h, k).start()

                @pl.when(jnp.logical_and(turn > 0, jnp.logical_not(piecewise(turn))))
                def _():
                    for br in branches:
                        for k in range(1, parts):
                            saved_copy(br, turn, k).start()

    def send_tops(first, end):
        @pl.loop(first, end)
        def _(m):
            @pl.when(jnp.logical_and(helper(m) == section, owner(m) == me))
            def _():
                for br in branches:
                    br.lifted[m // sections] = br.top[me, lax.rem(m, size)]
                    for k in range(1, parts):
                        top_copy(br, m, k).start()

    def wait_top(br, m):
        @pl.when(owner(m) != me)
        def _():
            drain(br.lifted.at[m // sections], br.top_got.at[m // sections])

    def lift(first, end):
        @pl.loop(first, end)
        def _(m):
            @pl.when(helper(m) == section)
            def _():
                for br in branches:
                    wait_top(br, m)
                    lift_copy(br, m).start()

    def partial_of(turn, at, length, got):
        first = turn * size + at

        @pl.when(owner(turn * size) != me)
        def _():
            for br in branches:
                drain(br.columns.at[turn, pl.ds(at, length)], br.saved_got.at[got])

        span = pl.ds(first, length)
        for br in branches:
            wide = br.columns.shape[-1]
            tokens = br.columns[turn, pl.ds(at, length)].reshape(-1, wide)

            def product(group):
                block = jnp.dot(tokens, br.weight[group], preferred_element_type=jnp.float32)
                return block.astype(jnp.bfloat16).reshape(length, -1, wide)

            for k in range(chips):
                br.pair_out[span, k] = product(other(ahead(k)))

            @pl.loop(first, first + length)
            def _(m):
                pair_copy(br, m).start()

            for k in range(chips):
                br.mine[span, k] = product(ahead(k))

    @jax.named_scope("partial")
    def partial(turn):
        partial_of(turn, 0, size, turn)

    def pair_sum(m):
        for br in branches:
            drain(br.pair_in.at[m], br.pair_got.at[m])
            for k in range(1, chips):
                both = br.mine[m, k].astype(jnp.float32) + br.pair_in[m, k].astype(jnp.float32)
                br.mine[m, k] = both.astype(jnp.bfloat16)
                chip_copy(br, m, k).start()

    def find_slope(br, m):
        total = br.mine[m, 0].astype(jnp.float32) + br.pair_in[m, 0].astype(jnp.float32)
        if chips > 1:
            drain(br.chip_in.at[m], br.chip_got.at[m])
        for k in range(1, chips):
            total = total + br.chip_in[m, k - 1].astype(jnp.float32)
        br.slopes[m, slot(me)] = gelu_slope(total).astype(jnp.bfloat16)

    @jax.named_scope("spread")
    def spread(m):
        at_hand = jnp.logical_and(is_last, helper(m) == section)
        for br in branches:
            find_slope(br, m)

            @pl.when(at_hand)
            def _():
                wait_top(br, m)
                br.above[m, slot(me)] = br.lifted[m // sections]

            @pl.when(jnp.logical_not(at_hand))
            def _():
                drain(br.below.at[m], br.above_got.at[m])

            upper = br.above[m, slot(me)].astype(jnp.float32)
            br.local[m, me] = (upper * br.slopes[m, slot(me)].astype(jnp.float32)).astype(jnp.bfloat16)
            for k in range(1, chips):
                far_copy(br, m, k).start()
            near_copy(br, m, 0).start()

    @jax.named_scope("relay")
    def relay(m):
        for br in branches:
            if chips > 1:
                drain(br.local.at[m, pl.ds(0, chips - 1)], br.far_got.at[m])
            for k in range(1, chips):
                near_copy(br, m, k).start()

    def through(br, m, blocks):
        total = jnp.dot(jnp.concatenate(blocks, axis=-1), br.flip[...], preferred_element_type=jnp.float32)
        total = br.above[m, slot(me)].astype(jnp.float32) + total
        br.below[m] = total.astype(jnp.bfloat16)

        @pl.when(jnp.logical_not(is_first))
        def _():
            hop_copy(br, m, 0).start()

        @pl.when(wide_out)
        def _():
            for k in range(1, chips):
                hop_copy(br, m, k).start()

    @jax.named_scope("descend")
    def descend(m):
        for br in branches:
            drain(br.local.at[m, pl.ds(0, chips)], br.near_got.at[m])
            through(br, m, [br.local[m, group] for group in range(parts)])

    @jax.named_scope("share")
    def share(m):
        for br in branches:
            drain(br.local.at[m, pl.ds(0, chips)], br.above_got.at[m])
            for k in range(chips):
                share_copy(br, m, k).start()

    @jax.named_scope("descend_wide")
    def descend_wide(m):
        for br in branches:
            drain(br.local.at[m, pl.ds(0, chips)], br.slope_got.at[m])
            drain(br.local.at[m, pl.ds(0, chips)], br.near_got.at[m])
            blocks = []
            for group in range(parts):
                block = br.above[m, group].astype(jnp.float32) * br.slopes[m, group].astype(jnp.float32)
                blocks.append(block.astype(jnp.bfloat16))
                br.local[m, group] = blocks[-1]
            through(br, m, blocks)

    def hand_out(m):
        for br in branches:
            @pl.when(owner(m) == me)
            def _():
                br.out[me, lax.rem(m, size)] = br.below[m]

            @pl.when(owner(m) != me)
            def _():
                out_copy(br, m).start()

    @jax.named_scope("sums")
    def add_sums(m):
        if not roomy:
            return
        turn, group = m // size - 1, lax.rem(m, size)

        @pl.when(turn >= 0)
        def _():
            span = pl.ds(lax.max(turn, 0) * size, size)
            for br in branches:
                wide = br.columns.shape[-1]
                left = br.columns[lax.max(turn, 0)].reshape(-1, wide)
                right = br.local[span, group].reshape(-1, wide)
                term = lax.dot_general(left, right, (((0,), (0,)), ((), ())), preferred_element_type=jnp.float32)
                br.sums[group] = br.sums[group] + (term * scale).astype(jnp.bfloat16).astype(jnp.float32)

                @pl.when(turn == parts - 2)
                def _():
                    pltpu.make_async_copy(br.sums.at[group], br.sums_out.at[group], sent(br, "sums")).start()

    early = min(sections, count)

    @pl.when(jnp.logical_not(is_last))
    def _():
        send_tops(0, early)

    send_saved(0, parts)

    @pl.when(is_last)
    def _():
        send_tops(0, early)

    send_tops(early, count)

    with jax.named_scope("regroup_weight"):
        for br in branches:
            rows = br.weight_in.shape[0]
            wide = br.weight.shape[-1]
            for group in range(parts):
                block = padded(br.weight_in[:, group * rows : (group + 1) * rows], wide)
                br.weight[group, :rows] = block
                if wide > rows:
                    br.weight[group, rows:] = jnp.zeros((wide - rows, wide), block.dtype)

    with jax.named_scope("flip_weight"):
        for br in branches:
            wide = br.weight.shape[-1]

            @pl.loop(0, parts)
            def _(group):
                br.flip[pl.ds(pl.multiple_of(group * wide, 128), wide), :] = br.weight[group].T
                if roomy:
                    br.sums[group] = jnp.zeros((wide, wide), jnp.float32)

    @pl.when(jnp.logical_not(is_last))
    def _():
        lift(0, early)

    @pl.loop(0, size // first_size)
    def _(h):
        with jax.named_scope("first_partial"):
            partial_of(0, h * first_size, first_size, h * parts)
        pl.loop(h * first_size, lax.min(first_sums, (h + 1) * first_size))(pair_sum)

    @pl.loop(0, max(size - 1, 1))
    def _(at):
        send_piece(at + chips * size)

    @pl.when(jnp.logical_not(is_last))
    def _():
        lift(early, count)
        pl.loop(1, parts)(partial)
        pl.loop(size, lax.max(first_sums, size))(pair_sum)

    def mixed(i):
        pair, at = i // (2 * size), lax.rem(i, 2 * size)
        return pair * 2 * size + lax.rem(at, 2) * size + at // 2

    def run_narrow():
        @pl.loop(0, count + lag + 1)
        def _(step):
            @pl.when(step < count)
            def _():
                spread(step)

            @pl.when(step < count - first_sums)
            def _():
                pair_sum(step + first_sums)

            @pl.when(step < size - max(size - 1, 1))
            def _():
                send_piece(chips * size + max(size - 1, 1) + step)

            @pl.when(jnp.logical_and(is_last, jnp.logical_and(step < count - size, lax.rem(step, size) == 0)))
            def _():
                partial(step // size + 1)

            @pl.when(jnp.logical_and(step > lag, step < count + lag + 1))
            def _():
                descend(step - lag - 1)

            @pl.when(jnp.logical_and(step >= lag, step < count + lag))
            def _():
                relay(step - lag)

            @pl.when(step > lag)
            def _():
                add_sums(step - lag - 1)

        pl.loop(0, count)(lambda i: hand_out(mixed(i)))

    def run_wide():
        def prepare(m):
            @pl.when(m < count)
            def _():
                for br in branches:
                    find_slope(br, m)
                    for k in range(1, chips):
                        slope_far(br, m, k).start()
                    slope_near(br, m, 0).start()

            @pl.when(m < count - first_sums)
            def _():
                pair_sum(m + first_sums)

            @pl.when(m >= 2)
            def _():
                for br in branches:
                    if chips > 1:
                        drain(br.local.at[m - 2, pl.ds(0, chips - 1)], br.far_got.at[m - 2])
                    for k in range(1, chips):
                        slope_near(br, m - 2, k).start()

        start = lax.min(10 + 2 * (wide_count - 1 - section), count + 2)
        with jax.named_scope("prepare"):
            pl.loop(0, start)(prepare)

        @pl.loop(0, count)
        def _(m):
            share(m)

            @pl.when(m > 0)
            def _():
                add_sums(lax.max(m - 1, 0))

            descend_wide(m)

            @pl.when(is_first)
            def _():
                hand_out(m)

            @pl.when(jnp.logical_and(section == 1, m >= size))
            def _():
                hand_out(mixed(lax.max(m - size, 0)))

            @pl.when(m + start < count + 2)
            def _():
                prepare(m + start)

        @pl.when(section == 1)
        def _():
            pl.loop(count - size, count)(lambda i: hand_out(mixed(i)))

        @pl.when(section > 1)
        def _():
            pl.loop(0, count)(lambda i: hand_out(mixed(i)))

        add_sums(count - 1)

    if roomy:
        pl.when(jnp.logical_not(wide_in))(run_narrow)
        pl.when(wide_in)(run_wide)
    else:
        run_narrow()

    with jax.named_scope("final_waits"):
        for br in branches:
            kept = br.columns_out.shape[0]
            columns = br.columns.at[pl.ds(parts - kept, kept)]
            pltpu.make_async_copy(columns, br.columns_out, sent(br, "columns")).start()
            local = br.local.at[pl.ds(count - kept * size, kept * size)]
            pltpu.make_async_copy(local, br.local_out, sent(br, "local")).start()
        for br in branches:
            others = pl.ds(0, parts - 1)
            drain(br.saved.at[others], sent(br, "saved"))
            drain(br.pair_in, sent(br, "pair"))
            drain(br.local.at[:, pl.ds(0, chips)], sent(br, "near"))
            if chips > 1:
                drain(br.chip_in, sent(br, "chip"))
                drain(br.local.at[:, pl.ds(0, chips - 1)], sent(br, "far"))

            if roomy:
                @pl.when(wide_in)
                def _():
                    drain(br.local.at[:, pl.ds(0, chips)], sent(br, "slope"))

                @pl.when(wide_out)
                def _():
                    drain(br.local.at[:, pl.ds(0, chips)], sent(br, "hop"))

                drain(br.sums, sent(br, "sums"))

            @pl.when(section > wide_count)
            def _():
                drain(br.below, sent(br, "hop"))

        @pl.loop(0, count)
        def _(m):
            @pl.when(jnp.logical_and(helper(m) == section, owner(m) == me))
            def _():
                for br in branches:
                    drain(br.top.at[pl.ds(0, parts - 1), 0], br.top_sent.at[m // sections])

            @pl.when(jnp.logical_and(jnp.logical_not(is_last), helper(m) == section))
            def _():
                for br in branches:
                    drain(br.lifted.at[m // sections], br.lift_sent.at[m // sections])

        for br in branches:
            drain(br.columns_out, sent(br, "columns"))
            drain(br.local_out, sent(br, "local"))
            drain(br.below.at[pl.ds(0, count - size)], sent(br, "out"))
            drain(br.out.at[pl.ds(0, parts - 1)], br.out_got.at[0])


def branch_call(sections, scale, weights, saveds, tops):
    half, full = jnp.bfloat16, jnp.float32
    operands, outs, out_specs, scratch = [], [], [], []
    vmem = pl.BlockSpec(memory_space=pltpu.VMEM)
    anywhere = pl.BlockSpec(memory_space=pl.ANY)
    rows, width = weights[0].shape
    parts = width // rows
    size, tokens = saveds[0].shape[:2]
    volume = sum(saved.size * saved.dtype.itemsize for saved in saveds)
    roomy = parts == size and volume * parts <= 8 * 1024 * 1024
    chips = parts // 2
    count = size * parts
    kept = 1 if roomy else parts
    turns = -(-count // sections)
    for weight, saved, top in zip(weights, saveds, tops):
        wide = -(-weight.shape[0] // 128) * 128
        operands += [weight, saved, top]
        all_sums = (parts, wide, wide) if roomy else (1, 8, 128)
        outs += [
            jax.ShapeDtypeStruct((parts, size, tokens, wide), half),
            jax.ShapeDtypeStruct((kept, size, tokens, wide), half),
            jax.ShapeDtypeStruct((kept * size, parts, tokens, wide), half),
            jax.ShapeDtypeStruct(all_sums, full),
        ]
        out_specs += [vmem, anywhere, anywhere, anywhere]
        dma = pltpu.SemaphoreType.DMA
        slots = parts if roomy else 1
        scratch += [
            pltpu.VMEM((parts, size, tokens, wide), half),
            pltpu.VMEM((parts, size, tokens, wide), half),
            pltpu.VMEM((turns, tokens, wide), half),
            pltpu.VMEM((parts, size, tokens, wide), half),
            pltpu.VMEM((count, parts, tokens, wide), half),
            pltpu.VMEM((parts, wide, wide), half),
            pltpu.VMEM((parts * wide, wide), half),
            pltpu.VMEM((count, slots, tokens, wide), half),
            pltpu.VMEM((count, tokens, wide), half),
            pltpu.VMEM((count, chips, tokens, wide), half),
            pltpu.VMEM((count, chips, tokens, wide), half),
            pltpu.VMEM((count, chips, tokens, wide), half),
            pltpu.VMEM((count, max(chips - 1, 1), tokens, wide), half),
            pltpu.VMEM((count, slots, tokens, wide), half),
            pltpu.VMEM(all_sums, full),
            dma((parts + 1,)),
            dma((count,)),
            dma((count,)),
            dma((count,)),
            dma((count,)),
            dma((count,)),
            dma((count if roomy else 1,)),
            dma((1,)),
            dma((len(SENDS),)),
            dma((turns,)),
            dma((turns,)),
            dma((turns,)),
        ]
    return roomy, pl.pallas_call(
        functools.partial(kernel, sections, parts, size, roomy, scale),
        out_shape=outs,
        in_specs=[vmem] * len(operands),
        out_specs=out_specs,
        scratch_shapes=scratch,
        compiler_params=pltpu.CompilerParams(
            collective_id=0, has_side_effects=True, vmem_limit_bytes=63 * 1024 * 1024
        ),
    )(*operands)


def finish_kernel(roomy, scale, *refs):
    outs, buffers, sems = refs[8:12], refs[12:16], refs[16]
    staged, in_sems = refs[17:25], refs[25]
    pending = []

    def load(i, *at):
        src, dst = (refs[i].at[at], staged[i].at[at]) if at else (refs[i], staged[i])
        return pltpu.make_async_copy(src, dst, in_sems.at[(i, *(at or (0,)))])

    def flush(src, dst):
        copy = pltpu.make_async_copy(src, dst, sems.at[len(pending)])
        copy.start()
        pending.append(copy)

    parts = staged[0].shape[0]
    for b in (1, 0):
        load(4 * b + 1).start()
        load(4 * b + 2).start()
        if roomy:
            for part in range(parts):
                load(4 * b + 3, part).start()
        load(4 * b).start()

    for b in (1, 0):
        grads_in, columns, local, sums_in = staged[4 * b : 4 * b + 4]
        grads, sums = outs[2 * b : 2 * b + 2]
        grad_buffer, sum_buffer = buffers[2 * b : 2 * b + 2]
        _, size, tokens, wide = grads_in.shape
        rows = sum_buffer.shape[0]
        load(4 * b + 1).wait()
        load(4 * b + 2).wait()
        spans = [slice(turn * size, (turn + 1) * size) for turn in range(columns.shape[0])]
        lefts = [columns[turn].reshape(size * tokens, wide)[:, :rows] for turn in range(columns.shape[0])]
        for part in range(parts):
            total = None
            for left, span in zip(lefts, spans):
                right = local[span, part].reshape(size * tokens, wide)[:, :rows]
                term = lax.dot_general(
                    left, right, (((0,), (0,)), ((), ())), preferred_element_type=jnp.float32,
                )
                term = (term * scale).astype(jnp.bfloat16).astype(jnp.float32)
                total = term if total is None else total + term
            if roomy:
                load(4 * b + 3, part).wait()
                total = sums_in[part, :rows, :rows] + total
            sum_buffer[:, part * rows : (part + 1) * rows] = total
            if rows % 128 == 0:
                span = pl.ds(part * rows, rows)
                flush(sum_buffer.at[:, span], sums.at[:, span])
        if rows % 128:
            flush(sum_buffer, sums)
        load(4 * b).wait()
        for part in range(parts):
            grad_buffer[:, :, part * rows : (part + 1) * rows] = grads_in[part][..., :rows]
        flush(grad_buffer, grads)
    for copy in pending:
        copy.wait()


def finish(roomy, results, rows_of, scale):
    outs, buffers = [], []
    for b in range(2):
        parts, size, tokens, _ = results[4 * b].shape
        rows = rows_of[b]
        shapes = [((size, tokens, parts * rows), jnp.bfloat16), ((rows, parts * rows), jnp.float32)]
        outs += [jax.ShapeDtypeStruct(*shape) for shape in shapes]
        buffers += [pltpu.VMEM(*shape) for shape in shapes]
    return pl.pallas_call(
        functools.partial(finish_kernel, roomy, scale),
        out_shape=outs,
        in_specs=[pl.BlockSpec(memory_space=pl.ANY)] * 8,
        out_specs=[pl.BlockSpec(memory_space=pl.ANY)] * 4,
        scratch_shapes=buffers
        + [pltpu.SemaphoreType.DMA((2 * parts + 4,))]
        + [pltpu.VMEM(result.shape, result.dtype) for result in results]
        + [pltpu.SemaphoreType.DMA((8, parts))],
        compiler_params=pltpu.CompilerParams(vmem_limit_bytes=63 * 1024 * 1024),
    )(*results)


def shards(vit_weight, t5_weight, vit_saved, t5_saved, vit_top_grad, t5_top_grad):
    sections = lax.axis_size("section")
    size, tokens = t5_top_grad.shape[:2]
    scale = 1.0 / (size * tokens)
    roomy, results = branch_call(
        sections,
        scale,
        [t5_weight[0], vit_weight[0]],
        [t5_saved[0], vit_saved[0]],
        [t5_top_grad, vit_top_grad],
    )
    t5_grads, t5_sum, vit_grads, vit_sum = finish(
        roomy, results, [t5_weight.shape[1], vit_weight.shape[1]], scale
    )
    return vit_grads[None], t5_grads[None], vit_sum[None], t5_sum[None]


def solution(mesh):
    placed = (
        P("section", "dp", None),
        P("section", "dp", None),
        P("section", None, "dp", None),
        P("section", None, "dp", None),
        P(None, "dp", None),
        P(None, "dp", None),
    )
    return jax.shard_map(
        shards,
        mesh=mesh,
        in_specs=placed,
        out_specs=(
            P("section", None, "dp", None),
            P("section", None, "dp", None),
            P("section", "dp", None),
            P("section", "dp", None),
        ),
        check_vma=False,
    )
```

```python
import functools

import jax
import jax.numpy as jnp
from jax import lax
from jax.experimental import pallas as pl
from jax.experimental.pallas import tpu as pltpu
from jax.sharding import PartitionSpec as P

root_half = 0.7071067811865476
inv_root_tau = 0.3989422804014327
MESH = pl.DeviceIdType.MESH


def gelu_slope(preact):
    cumulative = 0.5 * (1.0 + lax.erf(preact * root_half))
    density = jnp.exp(-0.5 * preact * preact) * inv_root_tau
    return cumulative + preact * density


NAMES = (
    "saved", "top", "lifted", "columns", "local", "weight", "flip", "above", "below", "mine",
    "pair_out", "pair_in", "chip_in", "slopes", "sums", "saved_got", "above_got", "pair_got",
    "chip_got", "near_got", "far_got", "slope_got", "out_got", "sent", "top_sent", "top_got",
    "lift_sent",
)
SENDS = ("saved", "pair", "chip", "near", "far", "slope", "hop", "out", "columns", "local", "sums")


class Branch:
    def __init__(self, ins, outs, scratch):
        self.weight_in, self.saved_in, self.top_in = ins
        self.out, self.columns_out, self.local_out, self.sums_out = outs
        for name, ref in zip(NAMES, scratch):
            setattr(self, name, ref)
        self.rows = self.weight_in.shape[0]
        self.tokens = self.saved_in.shape[1]
        self.main, self.rest = layout(self.rows, self.tokens)


def layout(rows, tokens):
    main = rows // 128 * 128
    rest = rows - main
    if rest and main and main % rest == 0 and tokens % (8 * (main // rest)) == 0:
        return main, rest
    return -(-rows // 128) * 128, 0


def fold(block, rest):
    if rest == 0:
        return block
    main = block.shape[1] - rest
    step = block.shape[0] * rest // main
    pieces = [block[first : first + step, main:] for first in range(0, block.shape[0], step)]
    return jnp.concatenate([block[:, :main], jnp.concatenate(pieces, axis=1)], axis=0)


def unfold(block, rest):
    if rest == 0:
        return [block]
    main = block.shape[1]
    tokens = block.shape[0] * main // (main + rest)
    tail = block[tokens:].astype(jnp.float32)
    pieces = [tail[:, first : first + rest] for first in range(0, main, rest)]
    return [block[:tokens], jnp.concatenate(pieces, axis=0).astype(block.dtype)]


def drain(ref, sem):
    pltpu.make_async_copy(ref, ref, sem).wait()


def kernel(sections, parts, size, roomy, scale, *refs):
    ins, outs, scratch = refs[:6], refs[6:14], refs[14:]
    branches = [
        Branch(ins[3 * b : 3 * b + 3], outs[4 * b : 4 * b + 4],
               scratch[len(NAMES) * b : len(NAMES) * (b + 1)])
        for b in range(2)
    ]
    count = size * parts
    first_size = size // 2 if size % 2 == 0 else size
    section = lax.axis_index("section")
    me = lax.axis_index("dp")
    chips = parts // 2
    chip, core = me // 2, me % 2
    partner = chip * 2 + 1 - core
    last = sections - 1
    is_last = section == last
    is_first = section == 0
    wide_count = sections // 2 + 1 if roomy else 0
    wide_flag = lax.min(lax.max(wide_count - section, 0), 1)
    wide_in = section < wide_count
    wide_out = jnp.logical_and(section > 0, section <= wide_count)
    lag = lax.min(1 + (1 - 1) * lax.max(section - last + 1, 0), count)
    narrow_sums = lax.min(3 + 4 * (last - section) * (last - section), count)
    first_sums = narrow_sums + (min(4, count) - narrow_sums) * wide_flag

    def slot(part):
        return part if roomy else 0

    def ahead(k):
        return lax.rem(chip + k, chips) * 2 + core

    def behind(k):
        return lax.rem(chip + chips - k, chips) * 2 + core

    def other(group):
        return group + 1 - 2 * core

    def owner(m):
        turn = m // size
        return lax.rem(turn, chips) * 2 + 1 - turn // chips

    def copy(src, dst, sent, got, where, part):
        return pltpu.make_async_remote_copy(
            src_ref=src, dst_ref=dst, send_sem=sent, recv_sem=got,
            device_id=(where, part), device_id_type=MESH,
        )

    def sent(br, name):
        return br.sent.at[SENDS.index(name)]

    def padded(block, wide):
        spare = wide - block.shape[-1]
        if spare:
            block = jnp.concatenate([block, jnp.zeros((*block.shape[:-1], spare), block.dtype)], axis=-1)
        return block

    def packed(br, block):
        return fold(block[:, : br.rows], br.rest) if br.rest else padded(block, br.main)

    def regroup(source, groups):
        cut = source.shape[-1] // parts
        for group in range(parts):
            groups[group] = padded(source[..., group * cut : (group + 1) * cut], groups.shape[-1])

    barrier = pltpu.get_barrier_semaphore()
    for k in range(1, parts):
        pl.semaphore_signal(barrier, inc=1, device_id=(section, lax.rem(me + k, parts)), device_id_type=MESH)

    def greet(other_section):
        for part in range(parts):
            pl.semaphore_signal(barrier, inc=1, device_id=(other_section, part), device_id_type=MESH)

    @pl.when(is_last)
    def _():
        @pl.loop(0, last)
        def _(lower):
            pl.semaphore_signal(barrier, inc=1, device_id=(lower, me), device_id_type=MESH)

    @pl.when(jnp.logical_not(is_last))
    def _():
        greet(section + 1)

    with jax.named_scope("regroup_saved"):
        for br in branches:
            regroup(br.saved_in, br.saved)
            for group in range(parts):
                for at in range(size):
                    block = br.top_in[at, :, group * br.rows : (group + 1) * br.rows]
                    br.top[group, at] = packed(br, block.astype(jnp.float32)).astype(jnp.bfloat16)
    greeted = parts * lax.min(section, 1) + lax.min(last - section, 1)
    with jax.named_scope("barrier"):
        pl.semaphore_wait(barrier, parts - 1 + greeted)

    def helper(m):
        return last - lax.rem(m, sections)

    def saved_copy(br, turn, k):
        to = lax.rem(me + k, parts)
        return copy(br.saved.at[to], br.columns.at[turn], sent(br, "saved"), br.saved_got.at[turn], section, to)

    def top_copy(br, m, k):
        to, turn = lax.rem(me + k, parts), m // sections
        return copy(br.top.at[to, lax.rem(m, size)], br.lifted.at[turn], br.top_sent.at[turn], br.top_got.at[turn], section, to)

    def lift_copy(br, m):
        turn = m // sections
        return copy(br.lifted.at[turn], br.above.at[m, slot(me)], br.lift_sent.at[turn], br.above_got.at[m], last, me)

    def pair_copy(br, m):
        return copy(br.pair_out.at[m], br.pair_in.at[m], sent(br, "pair"), br.pair_got.at[m], section, partner)

    def chip_copy(br, m, k):
        return copy(br.mine.at[m, k], br.chip_in.at[m, k - 1], sent(br, "chip"), br.chip_got.at[m], section, ahead(k))

    def near_copy(br, m, k):
        group = behind(k)
        return copy(br.local.at[m, group], br.local.at[m, group], sent(br, "near"), br.near_got.at[m], section, partner)

    def far_copy(br, m, k):
        return copy(br.local.at[m, me], br.local.at[m, me], sent(br, "far"), br.far_got.at[m], section, ahead(k))

    def hop_copy(br, m, k):
        return copy(br.below.at[m], br.above.at[m, slot(me)], sent(br, "hop"), br.above_got.at[m], lax.max(section - 1, 0), ahead(k))

    def share_copy(br, m, k):
        group = behind(k)
        return copy(br.above.at[m, group], br.above.at[m, group], sent(br, "near"), br.near_got.at[m], section, partner)

    def slope_far(br, m, k):
        return copy(br.slopes.at[m, me], br.slopes.at[m, me], sent(br, "far"), br.far_got.at[m], section, ahead(k))

    def slope_near(br, m, k):
        group = behind(k)
        return copy(br.slopes.at[m, group], br.slopes.at[m, group], sent(br, "slope"), br.slope_got.at[m], section, partner)

    def out_copy(br, m):
        return copy(br.below.at[m], br.out.at[me, lax.rem(m, size)], sent(br, "out"), br.out_got.at[0], section, owner(m))

    def half_copy(br, h, k):
        to, span = lax.rem(me + k, parts), pl.ds(h * first_size, first_size)
        return copy(br.saved.at[to, span], br.columns.at[0, span], sent(br, "saved"), br.saved_got.at[h * parts], section, to)

    def piecewise(turn):
        return jnp.logical_and(is_last, turn == chips)

    def piece_copy(br, m, k):
        to, turn, at = lax.rem(me + k, parts), m // size, lax.rem(m, size)
        return copy(br.saved.at[to, at], br.columns.at[turn, at], sent(br, "saved"), br.saved_got.at[turn], section, to)

    def send_piece(m):
        @pl.when(jnp.logical_and(piecewise(m // size), owner(m) == me))
        def _():
            for br in branches:
                for k in range(1, parts):
                    piece_copy(br, m, k).start()

    def send_saved(first, end):
        @pl.loop(first, end)
        def _(turn):
            @pl.when(owner(turn * size) == me)
            def _():
                for br in branches:
                    br.columns[turn] = br.saved[me]

                @pl.when(turn == 0)
                def _():
                    @pl.loop(0, size // first_size)
                    def _(h):
                        for br in branches:
                            for k in range(1, parts):
                                half_copy(br, h, k).start()

                @pl.when(jnp.logical_and(turn > 0, jnp.logical_not(piecewise(turn))))
                def _():
                    for br in branches:
                        for k in range(1, parts):
                            saved_copy(br, turn, k).start()

    def send_tops(first, end):
        @pl.loop(first, end)
        def _(m):
            @pl.when(jnp.logical_and(helper(m) == section, owner(m) == me))
            def _():
                for br in branches:
                    br.lifted[m // sections] = br.top[me, lax.rem(m, size)]
                    for k in range(1, parts):
                        top_copy(br, m, k).start()

    def wait_top(br, m):
        @pl.when(owner(m) != me)
        def _():
            drain(br.lifted.at[m // sections], br.top_got.at[m // sections])

    def lift(first, end):
        @pl.loop(first, end)
        def _(m):
            @pl.when(helper(m) == section)
            def _():
                for br in branches:
                    wait_top(br, m)
                    lift_copy(br, m).start()

    def partial_of(turn, at, length, got):
        first = turn * size + at

        @pl.when(owner(turn * size) != me)
        def _():
            for br in branches:
                drain(br.columns.at[turn, pl.ds(at, length)], br.saved_got.at[got])

        for br in branches:
            wide = br.columns.shape[-1]
            tokens = br.columns[turn, pl.ds(at, length)].reshape(-1, wide)

            def product(into, k, group):
                block = jnp.dot(tokens, br.weight[group], preferred_element_type=jnp.float32)
                for i in range(length):
                    piece = packed(br, block[i * br.tokens : (i + 1) * br.tokens])
                    into[first + i, k] = piece.astype(jnp.bfloat16)

            for k in range(chips):
                product(br.pair_out, k, other(ahead(k)))

            @pl.loop(first, first + length)
            def _(m):
                pair_copy(br, m).start()

            for k in range(chips):
                product(br.mine, k, ahead(k))

    @jax.named_scope("partial")
    def partial(turn):
        partial_of(turn, 0, size, turn)

    def pair_sum(m):
        for br in branches:
            drain(br.pair_in.at[m], br.pair_got.at[m])
            for k in range(1, chips):
                both = br.mine[m, k].astype(jnp.float32) + br.pair_in[m, k].astype(jnp.float32)
                br.mine[m, k] = both.astype(jnp.bfloat16)
                chip_copy(br, m, k).start()

    def find_slope(br, m):
        total = br.mine[m, 0].astype(jnp.float32) + br.pair_in[m, 0].astype(jnp.float32)
        if chips > 1:
            drain(br.chip_in.at[m], br.chip_got.at[m])
        for k in range(1, chips):
            total = total + br.chip_in[m, k - 1].astype(jnp.float32)
        br.slopes[m, slot(me)] = gelu_slope(total).astype(jnp.bfloat16)

    @jax.named_scope("spread")
    def spread(m):
        at_hand = jnp.logical_and(is_last, helper(m) == section)
        for br in branches:
            find_slope(br, m)

            @pl.when(at_hand)
            def _():
                wait_top(br, m)
                br.above[m, slot(me)] = br.lifted[m // sections]

            @pl.when(jnp.logical_not(at_hand))
            def _():
                drain(br.below.at[m], br.above_got.at[m])

            upper = br.above[m, slot(me)].astype(jnp.float32)
            br.local[m, me] = (upper * br.slopes[m, slot(me)].astype(jnp.float32)).astype(jnp.bfloat16)
            for k in range(1, chips):
                far_copy(br, m, k).start()
            near_copy(br, m, 0).start()

    @jax.named_scope("relay")
    def relay(m):
        for br in branches:
            if chips > 1:
                drain(br.local.at[m, pl.ds(0, chips - 1)], br.far_got.at[m])
            for k in range(1, chips):
                near_copy(br, m, k).start()

    def through(br, m, blocks):
        pieces = zip(*(unfold(block, br.rest) for block in blocks))
        blocks = [block for piece in pieces for block in piece]
        total = jnp.dot(jnp.concatenate(blocks, axis=-1), br.flip[...], preferred_element_type=jnp.float32)
        total = br.above[m, slot(me)].astype(jnp.float32) + packed(br, total)
        br.below[m] = total.astype(jnp.bfloat16)

        @pl.when(jnp.logical_not(is_first))
        def _():
            hop_copy(br, m, 0).start()

        @pl.when(wide_out)
        def _():
            for k in range(1, chips):
                hop_copy(br, m, k).start()

    @jax.named_scope("descend")
    def descend(m):
        for br in branches:
            drain(br.local.at[m, pl.ds(0, chips)], br.near_got.at[m])
            through(br, m, [br.local[m, group] for group in range(parts)])

    @jax.named_scope("share")
    def share(m):
        for br in branches:
            drain(br.local.at[m, pl.ds(0, chips)], br.above_got.at[m])
            for k in range(chips):
                share_copy(br, m, k).start()

    @jax.named_scope("descend_wide")
    def descend_wide(m):
        for br in branches:
            drain(br.local.at[m, pl.ds(0, chips)], br.slope_got.at[m])
            drain(br.local.at[m, pl.ds(0, chips)], br.near_got.at[m])
            blocks = []
            for group in range(parts):
                block = br.above[m, group].astype(jnp.float32) * br.slopes[m, group].astype(jnp.float32)
                blocks.append(block.astype(jnp.bfloat16))
                br.local[m, group] = blocks[-1]
            through(br, m, blocks)

    def hand_out(m):
        for br in branches:
            @pl.when(owner(m) == me)
            def _():
                br.out[me, lax.rem(m, size)] = br.below[m]

            @pl.when(owner(m) != me)
            def _():
                out_copy(br, m).start()

    @jax.named_scope("sums")
    def add_sums(m):
        if not roomy:
            return
        turn, group = m // size - 1, lax.rem(m, size)

        @pl.when(turn >= 0)
        def _():
            for br in branches:
                wide = br.columns.shape[-1]
                left = br.columns[lax.max(turn, 0)].reshape(-1, wide)
                turn_start = lax.max(turn, 0) * size
                right = jnp.concatenate(
                    [jnp.concatenate(unfold(br.local[turn_start + i, group], br.rest), axis=-1) for i in range(size)],
                    axis=0,
                )
                left, right = left[:, : br.rows], right[:, : br.rows]
                term = lax.dot_general(left, right, (((0,), (0,)), ((), ())), preferred_element_type=jnp.float32)
                br.sums[group] = br.sums[group] + (term * scale).astype(jnp.bfloat16).astype(jnp.float32)

                @pl.when(turn == parts - 2)
                def _():
                    pltpu.make_async_copy(br.sums.at[group], br.sums_out.at[group], sent(br, "sums")).start()

    early = min(sections, count)

    @pl.when(jnp.logical_not(is_last))
    def _():
        send_tops(0, early)

    send_saved(0, parts)

    @pl.when(is_last)
    def _():
        send_tops(0, early)

    send_tops(early, count)

    with jax.named_scope("regroup_weight"):
        for br in branches:
            rows = br.weight_in.shape[0]
            wide = br.weight.shape[-1]
            for group in range(parts):
                block = padded(br.weight_in[:, group * rows : (group + 1) * rows], wide)
                br.weight[group, :rows] = block
                if wide > rows:
                    br.weight[group, rows:] = jnp.zeros((wide - rows, wide), block.dtype)

    with jax.named_scope("flip_weight"):
        for br in branches:
            wide = br.weight.shape[-1]

            @pl.loop(0, parts)
            def _(group):
                turned = br.weight[group].T
                br.flip[pl.ds(pl.multiple_of(group * br.main, 128), br.main), :] = turned[: br.main]
                if br.rest:
                    at = pl.multiple_of(parts * br.main + group * br.rest, br.rest)
                    br.flip[pl.ds(at, br.rest), :] = turned[br.main : br.rows]
                if roomy:
                    br.sums[group] = jnp.zeros(br.sums.shape[1:], jnp.float32)

    @pl.when(jnp.logical_not(is_last))
    def _():
        lift(0, early)

    @pl.loop(0, size // first_size)
    def _(h):
        with jax.named_scope("first_partial"):
            partial_of(0, h * first_size, first_size, h * parts)
        pl.loop(h * first_size, lax.min(first_sums, (h + 1) * first_size))(pair_sum)

    @pl.loop(0, max(size - 1, 1))
    def _(at):
        send_piece(at + chips * size)

    @pl.when(jnp.logical_not(is_last))
    def _():
        lift(early, count)
        pl.loop(1, parts)(partial)
        pl.loop(size, lax.max(first_sums, size))(pair_sum)

    def mixed(i):
        pair, at = i // (2 * size), lax.rem(i, 2 * size)
        return pair * 2 * size + lax.rem(at, 2) * size + at // 2

    def run_narrow():
        @pl.loop(0, count + lag + 1)
        def _(step):
            @pl.when(step < count)
            def _():
                spread(step)

            @pl.when(step < count - first_sums)
            def _():
                pair_sum(step + first_sums)

            @pl.when(step < size - max(size - 1, 1))
            def _():
                send_piece(chips * size + max(size - 1, 1) + step)

            @pl.when(jnp.logical_and(is_last, jnp.logical_and(step < count - size, lax.rem(step, size) == 0)))
            def _():
                partial(step // size + 1)

            @pl.when(jnp.logical_and(step > lag, step < count + lag + 1))
            def _():
                descend(step - lag - 1)

            @pl.when(jnp.logical_and(step >= lag, step < count + lag))
            def _():
                relay(step - lag)

            @pl.when(step > lag)
            def _():
                add_sums(step - lag - 1)

        pl.loop(0, count)(lambda i: hand_out(mixed(i)))

    def run_wide():
        def prepare(m):
            @pl.when(m < count)
            def _():
                for br in branches:
                    find_slope(br, m)
                    for k in range(1, chips):
                        slope_far(br, m, k).start()
                    slope_near(br, m, 0).start()

            @pl.when(m < count - first_sums)
            def _():
                pair_sum(m + first_sums)

            @pl.when(m >= 2)
            def _():
                for br in branches:
                    if chips > 1:
                        drain(br.local.at[m - 2, pl.ds(0, chips - 1)], br.far_got.at[m - 2])
                    for k in range(1, chips):
                        slope_near(br, m - 2, k).start()

        start = lax.min(10 + 2 * (wide_count - 1 - section), count + 2)
        with jax.named_scope("prepare"):
            pl.loop(0, start)(prepare)

        @pl.loop(0, count)
        def _(m):
            share(m)

            @pl.when(m > 0)
            def _():
                add_sums(lax.max(m - 1, 0))

            descend_wide(m)

            @pl.when(is_first)
            def _():
                hand_out(m)

            @pl.when(jnp.logical_and(section == 1, m >= size))
            def _():
                hand_out(mixed(lax.max(m - size, 0)))

            @pl.when(m + start < count + 2)
            def _():
                prepare(m + start)

        @pl.when(section == 1)
        def _():
            pl.loop(count - size, count)(lambda i: hand_out(mixed(i)))

        @pl.when(section > 1)
        def _():
            pl.loop(0, count)(lambda i: hand_out(mixed(i)))

        add_sums(count - 1)

    if roomy:
        pl.when(jnp.logical_not(wide_in))(run_narrow)
        pl.when(wide_in)(run_wide)
    else:
        run_narrow()

    with jax.named_scope("final_waits"):
        for br in branches:
            kept = br.columns_out.shape[0]
            columns = br.columns.at[pl.ds(parts - kept, kept)]
            pltpu.make_async_copy(columns, br.columns_out, sent(br, "columns")).start()
            local = br.local.at[pl.ds(count - kept * size, kept * size)]
            pltpu.make_async_copy(local, br.local_out, sent(br, "local")).start()
        for br in branches:
            others = pl.ds(0, parts - 1)
            drain(br.saved.at[others], sent(br, "saved"))
            drain(br.pair_in, sent(br, "pair"))
            drain(br.local.at[:, pl.ds(0, chips)], sent(br, "near"))
            if chips > 1:
                drain(br.chip_in, sent(br, "chip"))
                drain(br.local.at[:, pl.ds(0, chips - 1)], sent(br, "far"))

            if roomy:
                @pl.when(wide_in)
                def _():
                    drain(br.local.at[:, pl.ds(0, chips)], sent(br, "slope"))

                @pl.when(wide_out)
                def _():
                    drain(br.local.at[:, pl.ds(0, chips)], sent(br, "hop"))

                drain(br.sums, sent(br, "sums"))

            @pl.when(section > wide_count)
            def _():
                drain(br.below, sent(br, "hop"))

        @pl.loop(0, count)
        def _(m):
            @pl.when(jnp.logical_and(helper(m) == section, owner(m) == me))
            def _():
                for br in branches:
                    drain(br.top.at[pl.ds(0, parts - 1), 0], br.top_sent.at[m // sections])

            @pl.when(jnp.logical_and(jnp.logical_not(is_last), helper(m) == section))
            def _():
                for br in branches:
                    drain(br.lifted.at[m // sections], br.lift_sent.at[m // sections])

        for br in branches:
            drain(br.columns_out, sent(br, "columns"))
            drain(br.local_out, sent(br, "local"))
            drain(br.below.at[pl.ds(0, count - size)], sent(br, "out"))
            drain(br.out.at[pl.ds(0, parts - 1)], br.out_got.at[0])


def branch_call(sections, scale, weights, saveds, tops):
    half, full = jnp.bfloat16, jnp.float32
    operands, outs, out_specs, scratch = [], [], [], []
    vmem = pl.BlockSpec(memory_space=pltpu.VMEM)
    anywhere = pl.BlockSpec(memory_space=pl.ANY)
    rows, width = weights[0].shape
    parts = width // rows
    size, tokens = saveds[0].shape[:2]
    volume = sum(saved.size * saved.dtype.itemsize for saved in saveds)
    roomy = parts == size and volume * parts <= 8 * 1024 * 1024
    chips = parts // 2
    count = size * parts
    kept = 1 if roomy else parts
    turns = -(-count // sections)
    for weight, saved, top in zip(weights, saveds, tops):
        rows = weight.shape[0]
        wide = -(-rows // 128) * 128
        main, rest = layout(rows, tokens)
        block = (tokens + tokens * rest // main, main)
        operands += [weight, saved, top]
        all_sums = (parts, rows, rows) if roomy else (1, 8, 128)
        outs += [
            jax.ShapeDtypeStruct((parts, size, *block), half),
            jax.ShapeDtypeStruct((kept, size, tokens, wide), half),
            jax.ShapeDtypeStruct((kept * size, parts, *block), half),
            jax.ShapeDtypeStruct(all_sums, full),
        ]
        out_specs += [vmem, anywhere, anywhere, anywhere]
        dma = pltpu.SemaphoreType.DMA
        slots = parts if roomy else 1
        scratch += [
            pltpu.VMEM((parts, size, tokens, wide), half),
            pltpu.VMEM((parts, size, *block), half),
            pltpu.VMEM((turns, *block), half),
            pltpu.VMEM((parts, size, tokens, wide), half),
            pltpu.VMEM((count, parts, *block), half),
            pltpu.VMEM((parts, wide, wide), half),
            pltpu.VMEM((parts * (main + rest), wide), half),
            pltpu.VMEM((count, slots, *block), half),
            pltpu.VMEM((count, *block), half),
            pltpu.VMEM((count, chips, *block), half),
            pltpu.VMEM((count, chips, *block), half),
            pltpu.VMEM((count, chips, *block), half),
            pltpu.VMEM((count, max(chips - 1, 1), *block), half),
            pltpu.VMEM((count, slots, *block), half),
            pltpu.VMEM(all_sums, full),
            dma((parts + 1,)),
            dma((count,)),
            dma((count,)),
            dma((count,)),
            dma((count,)),
            dma((count,)),
            dma((count if roomy else 1,)),
            dma((1,)),
            dma((len(SENDS),)),
            dma((turns,)),
            dma((turns,)),
            dma((turns,)),
        ]
    return roomy, pl.pallas_call(
        functools.partial(kernel, sections, parts, size, roomy, scale),
        out_shape=outs,
        in_specs=[vmem] * len(operands),
        out_specs=out_specs,
        scratch_shapes=scratch,
        compiler_params=pltpu.CompilerParams(
            collective_id=0, has_side_effects=True, vmem_limit_bytes=63 * 1024 * 1024
        ),
    )(*operands)


def finish_kernel(roomy, scale, *refs):
    outs, buffers, sems = refs[8:12], refs[12:16], refs[16]
    staged, in_sems = refs[17:25], refs[25]
    pending = []

    def load(i, *at):
        src, dst = (refs[i].at[at], staged[i].at[at]) if at else (refs[i], staged[i])
        return pltpu.make_async_copy(src, dst, in_sems.at[(i, *(at or (0,)))])

    def flush(src, dst):
        copy = pltpu.make_async_copy(src, dst, sems.at[len(pending)])
        copy.start()
        pending.append(copy)

    parts = staged[0].shape[0]
    for b in (1, 0):
        load(4 * b + 1).start()
        load(4 * b + 2).start()
        if roomy:
            for part in range(parts):
                load(4 * b + 3, part).start()
        load(4 * b).start()

    for b in (1, 0):
        grads_in, columns, local, sums_in = staged[4 * b : 4 * b + 4]
        grads, sums = outs[2 * b : 2 * b + 2]
        grad_buffer, sum_buffer = buffers[2 * b : 2 * b + 2]
        size, tokens = grad_buffer.shape[:2]
        wide = columns.shape[-1]
        rows = sum_buffer.shape[0]
        rest = layout(rows, tokens)[1]

        def whole(block):
            return jnp.concatenate(unfold(block, rest), axis=-1)[:, :rows]

        load(4 * b + 1).wait()
        load(4 * b + 2).wait()
        spans = [range(turn * size, (turn + 1) * size) for turn in range(columns.shape[0])]
        lefts = [columns[turn].reshape(size * tokens, wide)[:, :rows] for turn in range(columns.shape[0])]
        for part in range(parts):
            total = None
            for left, span in zip(lefts, spans):
                right = jnp.concatenate([whole(local[i, part]) for i in span], axis=0)
                term = lax.dot_general(
                    left, right, (((0,), (0,)), ((), ())), preferred_element_type=jnp.float32,
                )
                term = (term * scale).astype(jnp.bfloat16).astype(jnp.float32)
                total = term if total is None else total + term
            if roomy:
                load(4 * b + 3, part).wait()
                total = sums_in[part] + total
            sum_buffer[:, part * rows : (part + 1) * rows] = total
            if rows % 128 == 0:
                span = pl.ds(part * rows, rows)
                flush(sum_buffer.at[:, span], sums.at[:, span])
        if rows % 128:
            flush(sum_buffer, sums)
        load(4 * b).wait()
        for part in range(parts):
            for at in range(size):
                grad_buffer[at, :, part * rows : (part + 1) * rows] = whole(grads_in[part, at])
        flush(grad_buffer, grads)
    for copy in pending:
        copy.wait()


def finish(roomy, results, sizes, rows_of, scale):
    outs, buffers = [], []
    for b in range(2):
        parts = results[4 * b].shape[0]
        size, tokens = sizes
        rows = rows_of[b]
        shapes = [((size, tokens, parts * rows), jnp.bfloat16), ((rows, parts * rows), jnp.float32)]
        outs += [jax.ShapeDtypeStruct(*shape) for shape in shapes]
        buffers += [pltpu.VMEM(*shape) for shape in shapes]
    return pl.pallas_call(
        functools.partial(finish_kernel, roomy, scale),
        out_shape=outs,
        in_specs=[pl.BlockSpec(memory_space=pl.ANY)] * 8,
        out_specs=[pl.BlockSpec(memory_space=pl.ANY)] * 4,
        scratch_shapes=buffers
        + [pltpu.SemaphoreType.DMA((2 * parts + 4,))]
        + [pltpu.VMEM(result.shape, result.dtype) for result in results]
        + [pltpu.SemaphoreType.DMA((8, parts))],
        compiler_params=pltpu.CompilerParams(vmem_limit_bytes=63 * 1024 * 1024),
    )(*results)


def shards(vit_weight, t5_weight, vit_saved, t5_saved, vit_top_grad, t5_top_grad):
    sections = lax.axis_size("section")
    size, tokens = t5_top_grad.shape[:2]
    scale = 1.0 / (size * tokens)
    roomy, results = branch_call(
        sections,
        scale,
        [t5_weight[0], vit_weight[0]],
        [t5_saved[0], vit_saved[0]],
        [t5_top_grad, vit_top_grad],
    )
    t5_grads, t5_sum, vit_grads, vit_sum = finish(
        roomy, results, (size, tokens), [t5_weight.shape[1], vit_weight.shape[1]], scale
    )
    return vit_grads[None], t5_grads[None], vit_sum[None], t5_sum[None]


def solution(mesh):
    placed = (
        P("section", "dp", None),
        P("section", "dp", None),
        P("section", None, "dp", None),
        P("section", None, "dp", None),
        P(None, "dp", None),
        P(None, "dp", None),
    )
    return jax.shard_map(
        shards,
        mesh=mesh,
        in_specs=placed,
        out_specs=(
            P("section", None, "dp", None),
            P("section", None, "dp", None),
            P("section", "dp", None),
            P("section", "dp", None),
        ),
        check_vma=False,
    )
```

```python
import functools

import jax
import jax.numpy as jnp
from jax import lax
from jax.experimental import pallas as pl
from jax.experimental.pallas import tpu as pltpu
from jax.sharding import PartitionSpec as P

root_half = 0.7071067811865476
inv_root_tau = 0.3989422804014327
MESH = pl.DeviceIdType.MESH


def gelu_slope(preact):
    cumulative = 0.5 * (1.0 + lax.erf(preact * root_half))
    density = jnp.exp(-0.5 * preact * preact) * inv_root_tau
    return cumulative + preact * density


NAMES = (
    "saved", "top", "lifted", "columns", "local", "weight", "flip", "above", "below", "mine",
    "pair_out", "pair_in", "chip_in", "slopes", "sums", "saved_got", "above_got", "pair_got",
    "chip_got", "near_got", "far_got", "slope_got", "out_got", "sent", "top_sent", "top_got",
    "lift_sent",
    "weight_raw", "top_raw", "raw_got",
)
SENDS = ("saved", "pair", "chip", "near", "far", "slope", "hop", "out", "columns", "local", "sums")


class Branch:
    def __init__(self, ins, outs, scratch):
        self.weight_in, self.saved_in, self.top_in = ins
        self.out, self.columns_out, self.local_out, self.sums_out = outs
        for name, ref in zip(NAMES, scratch):
            setattr(self, name, ref)
        self.rows = self.weight_in.shape[0]
        self.tokens = self.saved_in.shape[1]
        self.main, self.rest = layout(self.rows, self.tokens)


def layout(rows, tokens):
    main = rows // 128 * 128
    rest = rows - main
    if rest and main and main % rest == 0 and tokens % (8 * (main // rest)) == 0:
        return main, rest
    return -(-rows // 128) * 128, 0


def fold(block, rest):
    if rest == 0:
        return block
    main = block.shape[1] - rest
    step = block.shape[0] * rest // main
    pieces = [block[first : first + step, main:] for first in range(0, block.shape[0], step)]
    return jnp.concatenate([block[:, :main], jnp.concatenate(pieces, axis=1)], axis=0)


def unfold(block, rest):
    if rest == 0:
        return [block]
    main = block.shape[1]
    tokens = block.shape[0] * main // (main + rest)
    tail = block[tokens:].astype(jnp.float32)
    pieces = [tail[:, first : first + rest] for first in range(0, main, rest)]
    return [block[:tokens], jnp.concatenate(pieces, axis=0).astype(block.dtype)]


def drain(ref, sem):
    pltpu.make_async_copy(ref, ref, sem).wait()


def kernel(sections, parts, size, roomy, scale, *refs):
    ins, outs, scratch = refs[:6], refs[6:14], refs[14:]
    branches = [
        Branch(ins[3 * b : 3 * b + 3], outs[4 * b : 4 * b + 4],
               scratch[len(NAMES) * b : len(NAMES) * (b + 1)])
        for b in range(2)
    ]
    count = size * parts
    first_size = size // 2 if size % 2 == 0 else size
    section = lax.axis_index("section")
    me = lax.axis_index("dp")
    chips = parts // 2
    chip, core = me // 2, me % 2
    partner = chip * 2 + 1 - core
    last = sections - 1
    is_last = section == last
    is_first = section == 0
    wide_count = sections // 2 + 1 if roomy else 0
    wide_flag = lax.min(lax.max(wide_count - section, 0), 1)
    wide_in = section < wide_count
    wide_out = jnp.logical_and(section > 0, section <= wide_count)
    lag = lax.min(1 + (1 - 1) * lax.max(section - last + 1, 0), count)
    narrow_sums = lax.min(3 + 4 * (last - section) * (last - section), count)
    first_sums = narrow_sums + (min(4, count) - narrow_sums) * wide_flag

    def slot(part):
        return part if roomy else 0

    def ahead(k):
        return lax.rem(chip + k, chips) * 2 + core

    def behind(k):
        return lax.rem(chip + chips - k, chips) * 2 + core

    def other(group):
        return group + 1 - 2 * core

    def owner(m):
        turn = m // size
        return lax.rem(turn, chips) * 2 + 1 - turn // chips

    def copy(src, dst, sent, got, where, part):
        return pltpu.make_async_remote_copy(
            src_ref=src, dst_ref=dst, send_sem=sent, recv_sem=got,
            device_id=(where, part), device_id_type=MESH,
        )

    def sent(br, name):
        return br.sent.at[SENDS.index(name)]

    def padded(block, wide):
        spare = wide - block.shape[-1]
        if spare:
            block = jnp.concatenate([block, jnp.zeros((*block.shape[:-1], spare), block.dtype)], axis=-1)
        return block

    def packed(br, block):
        return fold(block[:, : br.rows], br.rest) if br.rest else padded(block, br.main)

    def regroup(source, groups):
        cut = source.shape[-1] // parts
        for group in range(parts):
            groups[group] = padded(source[..., group * cut : (group + 1) * cut], groups.shape[-1])

    def weight_load(br):
        return pltpu.make_async_copy(br.weight_in, br.weight_raw, br.raw_got.at[0])

    def top_load(br):
        return pltpu.make_async_copy(br.top_in, br.top_raw, br.raw_got.at[1])

    for br in branches:
        top_load(br).start()
    for br in branches:
        weight_load(br).start()

    barrier = pltpu.get_barrier_semaphore()
    for k in range(1, parts):
        pl.semaphore_signal(barrier, inc=1, device_id=(section, lax.rem(me + k, parts)), device_id_type=MESH)

    def greet(other_section):
        for part in range(parts):
            pl.semaphore_signal(barrier, inc=1, device_id=(other_section, part), device_id_type=MESH)

    @pl.when(is_last)
    def _():
        @pl.loop(0, last)
        def _(lower):
            pl.semaphore_signal(barrier, inc=1, device_id=(lower, me), device_id_type=MESH)

    @pl.when(jnp.logical_not(is_last))
    def _():
        greet(section + 1)

    with jax.named_scope("regroup_saved"):
        for br in branches:
            regroup(br.saved_in, br.saved)
        for br in branches:
            top_load(br).wait()
            for group in range(parts):
                for at in range(size):
                    block = br.top_raw[at, :, group * br.rows : (group + 1) * br.rows]
                    br.top[group, at] = packed(br, block.astype(jnp.float32)).astype(jnp.bfloat16)
    greeted = parts * lax.min(section, 1) + lax.min(last - section, 1)
    with jax.named_scope("barrier"):
        pl.semaphore_wait(barrier, parts - 1 + greeted)

    def helper(m):
        return last - lax.rem(m, sections)

    def saved_copy(br, turn, k):
        to = lax.rem(me + k, parts)
        return copy(br.saved.at[to], br.columns.at[turn], sent(br, "saved"), br.saved_got.at[turn], section, to)

    def top_copy(br, m, k):
        to, turn = lax.rem(me + k, parts), m // sections
        return copy(br.top.at[to, lax.rem(m, size)], br.lifted.at[turn], br.top_sent.at[turn], br.top_got.at[turn], section, to)

    def lift_copy(br, m):
        turn = m // sections
        return copy(br.lifted.at[turn], br.above.at[m, slot(me)], br.lift_sent.at[turn], br.above_got.at[m], last, me)

    def pair_copy(br, m):
        return copy(br.pair_out.at[m], br.pair_in.at[m], sent(br, "pair"), br.pair_got.at[m], section, partner)

    def chip_copy(br, m, k):
        return copy(br.mine.at[m, k], br.chip_in.at[m, k - 1], sent(br, "chip"), br.chip_got.at[m], section, ahead(k))

    def near_copy(br, m, k):
        group = behind(k)
        return copy(br.local.at[m, group], br.local.at[m, group], sent(br, "near"), br.near_got.at[m], section, partner)

    def far_copy(br, m, k):
        return copy(br.local.at[m, me], br.local.at[m, me], sent(br, "far"), br.far_got.at[m], section, ahead(k))

    def hop_copy(br, m, k):
        return copy(br.below.at[m], br.above.at[m, slot(me)], sent(br, "hop"), br.above_got.at[m], lax.max(section - 1, 0), ahead(k))

    def share_copy(br, m, k):
        group = behind(k)
        return copy(br.above.at[m, group], br.above.at[m, group], sent(br, "near"), br.near_got.at[m], section, partner)

    def slope_far(br, m, k):
        return copy(br.slopes.at[m, me], br.slopes.at[m, me], sent(br, "far"), br.far_got.at[m], section, ahead(k))

    def slope_near(br, m, k):
        group = behind(k)
        return copy(br.slopes.at[m, group], br.slopes.at[m, group], sent(br, "slope"), br.slope_got.at[m], section, partner)

    def out_copy(br, m):
        return copy(br.below.at[m], br.out.at[me, lax.rem(m, size)], sent(br, "out"), br.out_got.at[0], section, owner(m))

    def half_copy(br, h, k):
        to, span = lax.rem(me + k, parts), pl.ds(h * first_size, first_size)
        return copy(br.saved.at[to, span], br.columns.at[0, span], sent(br, "saved"), br.saved_got.at[h * parts], section, to)

    def piecewise(turn):
        return jnp.logical_and(is_last, turn >= chips)

    def piece_copy(br, m, k):
        to, turn, at = lax.rem(me + k, parts), m // size, lax.rem(m, size)
        return copy(br.saved.at[to, at], br.columns.at[turn, at], sent(br, "saved"), br.saved_got.at[turn], section, to)

    def send_piece(m):
        @pl.when(jnp.logical_and(piecewise(m // size), owner(m) == me))
        def _():
            for br in branches:
                for k in range(1, parts):
                    piece_copy(br, m, k).start()

    def send_saved(first, end):
        @pl.loop(first, end)
        def _(turn):
            @pl.when(owner(turn * size) == me)
            def _():
                for br in branches:
                    br.columns[turn] = br.saved[me]

                @pl.when(turn == 0)
                def _():
                    @pl.loop(0, size // first_size)
                    def _(h):
                        for br in branches:
                            for k in range(1, parts):
                                half_copy(br, h, k).start()

                @pl.when(turn > chips)
                def _():
                    pl.loop(0, first_size)(lambda at: send_piece(turn * size + at))

                @pl.when(jnp.logical_and(turn > 0, jnp.logical_not(piecewise(turn))))
                def _():
                    for br in branches:
                        for k in range(1, parts):
                            saved_copy(br, turn, k).start()

    def send_tops(first, end):
        @pl.loop(first, end)
        def _(m):
            @pl.when(jnp.logical_and(helper(m) == section, owner(m) == me))
            def _():
                for br in branches:
                    br.lifted[m // sections] = br.top[me, lax.rem(m, size)]
                    for k in range(1, parts):
                        top_copy(br, m, k).start()

    def wait_top(br, m):
        @pl.when(owner(m) != me)
        def _():
            drain(br.lifted.at[m // sections], br.top_got.at[m // sections])

    def lift(first, end):
        @pl.loop(first, end)
        def _(m):
            @pl.when(helper(m) == section)
            def _():
                for br in branches:
                    wait_top(br, m)
                    lift_copy(br, m).start()

    def partial_of(turn, at, length, got):
        first = turn * size + at

        @pl.when(owner(turn * size) != me)
        def _():
            for br in branches:
                drain(br.columns.at[turn, pl.ds(at, length)], br.saved_got.at[got])

        for br in branches:
            wide = br.columns.shape[-1]
            tokens = br.columns[turn, pl.ds(at, length)].reshape(-1, wide)

            def product(into, k, group):
                block = jnp.dot(tokens, br.weight[group], preferred_element_type=jnp.float32)
                for i in range(length):
                    piece = packed(br, block[i * br.tokens : (i + 1) * br.tokens])
                    into[first + i, k] = piece.astype(jnp.bfloat16)

            for k in range(chips):
                product(br.pair_out, k, other(ahead(k)))

            @pl.loop(first, first + length)
            def _(m):
                pair_copy(br, m).start()

            for k in range(chips):
                product(br.mine, k, ahead(k))

    @jax.named_scope("partial")
    def partial(turn):
        partial_of(turn, 0, size, turn)

    def pair_sum(m):
        for br in branches:
            drain(br.pair_in.at[m], br.pair_got.at[m])
            for k in range(1, chips):
                both = br.mine[m, k].astype(jnp.float32) + br.pair_in[m, k].astype(jnp.float32)
                br.mine[m, k] = both.astype(jnp.bfloat16)
                chip_copy(br, m, k).start()

    def find_slope(br, m):
        total = br.mine[m, 0].astype(jnp.float32) + br.pair_in[m, 0].astype(jnp.float32)
        if chips > 1:
            drain(br.chip_in.at[m], br.chip_got.at[m])
        for k in range(1, chips):
            total = total + br.chip_in[m, k - 1].astype(jnp.float32)
        br.slopes[m, slot(me)] = gelu_slope(total).astype(jnp.bfloat16)

    @jax.named_scope("spread")
    def spread(m):
        at_hand = jnp.logical_and(is_last, helper(m) == section)
        for br in branches:
            find_slope(br, m)

            @pl.when(at_hand)
            def _():
                wait_top(br, m)
                br.above[m, slot(me)] = br.lifted[m // sections]

            @pl.when(jnp.logical_not(at_hand))
            def _():
                drain(br.below.at[m], br.above_got.at[m])

            upper = br.above[m, slot(me)].astype(jnp.float32)
            br.local[m, me] = (upper * br.slopes[m, slot(me)].astype(jnp.float32)).astype(jnp.bfloat16)
            for k in range(1, chips):
                far_copy(br, m, k).start()
            near_copy(br, m, 0).start()

    @jax.named_scope("relay")
    def relay(m):
        for br in branches:
            if chips > 1:
                drain(br.local.at[m, pl.ds(0, chips - 1)], br.far_got.at[m])
            for k in range(1, chips):
                near_copy(br, m, k).start()

    def through(br, m, blocks):
        pieces = zip(*(unfold(block, br.rest) for block in blocks))
        blocks = [block for piece in pieces for block in piece]
        total = jnp.dot(jnp.concatenate(blocks, axis=-1), br.flip[...], preferred_element_type=jnp.float32)
        total = br.above[m, slot(me)].astype(jnp.float32) + packed(br, total)
        br.below[m] = total.astype(jnp.bfloat16)

        @pl.when(jnp.logical_not(is_first))
        def _():
            hop_copy(br, m, 0).start()

        @pl.when(wide_out)
        def _():
            for k in range(1, chips):
                hop_copy(br, m, k).start()

    @jax.named_scope("descend")
    def descend(m):
        for br in branches:
            drain(br.local.at[m, pl.ds(0, chips)], br.near_got.at[m])
            through(br, m, [br.local[m, group] for group in range(parts)])

    @jax.named_scope("share")
    def share(m):
        for br in branches:
            drain(br.local.at[m, pl.ds(0, chips)], br.above_got.at[m])
            for k in range(chips):
                share_copy(br, m, k).start()

    @jax.named_scope("descend_wide")
    def descend_wide(m):
        for br in branches:
            drain(br.local.at[m, pl.ds(0, chips)], br.slope_got.at[m])
            drain(br.local.at[m, pl.ds(0, chips)], br.near_got.at[m])
            blocks = []
            for group in range(parts):
                block = br.above[m, group].astype(jnp.float32) * br.slopes[m, group].astype(jnp.float32)
                blocks.append(block.astype(jnp.bfloat16))
                br.local[m, group] = blocks[-1]
            through(br, m, blocks)

    def hand_out(m):
        for br in branches:
            @pl.when(owner(m) == me)
            def _():
                br.out[me, lax.rem(m, size)] = br.below[m]

            @pl.when(owner(m) != me)
            def _():
                out_copy(br, m).start()

    @jax.named_scope("sums")
    def add_sums(m):
        if not roomy:
            return
        turn, group = m // size - 1, lax.rem(m, size)

        @pl.when(turn >= 0)
        def _():
            for br in branches:
                wide = br.columns.shape[-1]
                left = br.columns[lax.max(turn, 0)].reshape(-1, wide)
                turn_start = lax.max(turn, 0) * size
                right = jnp.concatenate(
                    [jnp.concatenate(unfold(br.local[turn_start + i, group], br.rest), axis=-1) for i in range(size)],
                    axis=0,
                )
                left, right = left[:, : br.rows], right[:, : br.rows]
                term = lax.dot_general(left, right, (((0,), (0,)), ((), ())), preferred_element_type=jnp.float32)
                total = br.sums[group] + (term * scale).astype(jnp.bfloat16).astype(jnp.float32)
                br.sums[group] = total

                @pl.when(turn == parts - 2)
                def _():
                    pltpu.make_async_copy(br.sums.at[group], br.sums_out.at[group], sent(br, "sums")).start()

    early = min(sections, count)

    @pl.when(jnp.logical_not(is_last))
    def _():
        send_tops(0, early)

    send_saved(0, parts)

    @pl.when(is_last)
    def _():
        send_tops(0, early)

    send_tops(early, count)

    with jax.named_scope("regroup_weight"):
        for br in branches:
            rows = br.weight_in.shape[0]
            wide = br.weight.shape[-1]
            weight_load(br).wait()
            for group in range(parts):
                block = padded(br.weight_raw[:, group * rows : (group + 1) * rows], wide)
                br.weight[group, :rows] = block
                if wide > rows:
                    br.weight[group, rows:] = jnp.zeros((wide - rows, wide), block.dtype)

    with jax.named_scope("flip_weight"):
        for br in branches:
            wide = br.weight.shape[-1]

            @pl.loop(0, parts)
            def _(group):
                turned = br.weight[group].T
                br.flip[pl.ds(pl.multiple_of(group * br.main, 128), br.main), :] = turned[: br.main]
                if br.rest:
                    at = pl.multiple_of(parts * br.main + group * br.rest, br.rest)
                    br.flip[pl.ds(at, br.rest), :] = turned[br.main : br.rows]
                if roomy:
                    br.sums[group] = jnp.zeros(br.sums.shape[1:], jnp.float32)

    @pl.when(jnp.logical_not(is_last))
    def _():
        lift(0, early)

    @pl.loop(0, size // first_size)
    def _(h):
        with jax.named_scope("first_partial"):
            partial_of(0, h * first_size, first_size, h * parts)
        pl.loop(h * first_size, lax.min(first_sums, (h + 1) * first_size))(pair_sum)

    @pl.loop(0, max(size - 1, 1))
    def _(at):
        send_piece(at + chips * size)

    @pl.loop(chips + 1, parts)
    def _(turn):
        pl.loop(first_size, size)(lambda at: send_piece(turn * size + at))

    @pl.when(jnp.logical_not(is_last))
    def _():
        lift(early, count)
        pl.loop(1, parts)(partial)
        pl.loop(size, lax.max(first_sums, size))(pair_sum)

    def mixed(i):
        pair, at = i // (2 * size), lax.rem(i, 2 * size)
        return pair * 2 * size + lax.rem(at, 2) * size + at // 2

    def run_narrow():
        @pl.loop(0, count + lag + 1)
        def _(step):
            @pl.when(step < count)
            def _():
                spread(step)

            @pl.when(step < count - first_sums)
            def _():
                pair_sum(step + first_sums)

            @pl.when(step < size - max(size - 1, 1))
            def _():
                send_piece(chips * size + max(size - 1, 1) + step)

            @pl.when(jnp.logical_and(is_last, jnp.logical_and(step < count - size, lax.rem(step, size) == 0)))
            def _():
                partial(step // size + 1)

            @pl.when(jnp.logical_and(step > lag, step < count + lag + 1))
            def _():
                descend(step - lag - 1)

            @pl.when(jnp.logical_and(step >= lag, step < count + lag))
            def _():
                relay(step - lag)

            @pl.when(step > lag)
            def _():
                add_sums(step - lag - 1)

        pl.loop(0, count)(lambda i: hand_out(mixed(i)))

    def run_wide():
        def prepare(m):
            @pl.when(m < count)
            def _():
                for br in branches:
                    find_slope(br, m)
                    for k in range(1, chips):
                        slope_far(br, m, k).start()
                    slope_near(br, m, 0).start()

            @pl.when(m < count - first_sums)
            def _():
                pair_sum(m + first_sums)

            @pl.when(m >= 2)
            def _():
                for br in branches:
                    if chips > 1:
                        drain(br.local.at[m - 2, pl.ds(0, chips - 1)], br.far_got.at[m - 2])
                    for k in range(1, chips):
                        slope_near(br, m - 2, k).start()

        start = lax.min(10 + 2 * (wide_count - 1 - section), count + 2)
        with jax.named_scope("prepare"):
            pl.loop(0, start)(prepare)

        @pl.loop(0, count)
        def _(m):
            share(m)

            @pl.when(m > 0)
            def _():
                add_sums(lax.max(m - 1, 0))

            descend_wide(m)

            @pl.when(is_first)
            def _():
                hand_out(m)

            @pl.when(jnp.logical_and(section == 1, jnp.logical_and(m >= size, m < count - size)))
            def _():
                hand_out(mixed(lax.max(m - size, 0)))

            @pl.when(m + start < count + 2)
            def _():
                prepare(m + start)

        @pl.when(section == 1)
        def _():
            pl.loop(max(count - 2 * size, 0), count)(lambda i: hand_out(mixed(i)))

        @pl.when(section > 1)
        def _():
            pl.loop(0, count)(lambda i: hand_out(mixed(i)))

        add_sums(count - 1)

    if roomy:
        pl.when(jnp.logical_not(wide_in))(run_narrow)
        pl.when(wide_in)(run_wide)
    else:
        run_narrow()

    with jax.named_scope("final_waits"):
        for br in branches:
            kept = br.columns_out.shape[0]
            columns = br.columns.at[pl.ds(parts - kept, kept)]
            pltpu.make_async_copy(columns, br.columns_out, sent(br, "columns")).start()
            local = br.local.at[pl.ds(count - kept * size, kept * size)]
            pltpu.make_async_copy(local, br.local_out, sent(br, "local")).start()
        for br in branches:
            others = pl.ds(0, parts - 1)
            drain(br.saved.at[others], sent(br, "saved"))
            drain(br.pair_in, sent(br, "pair"))
            drain(br.local.at[:, pl.ds(0, chips)], sent(br, "near"))
            if chips > 1:
                drain(br.chip_in, sent(br, "chip"))
                drain(br.local.at[:, pl.ds(0, chips - 1)], sent(br, "far"))

            if roomy:
                @pl.when(wide_in)
                def _():
                    drain(br.local.at[:, pl.ds(0, chips)], sent(br, "slope"))

                @pl.when(wide_out)
                def _():
                    drain(br.local.at[:, pl.ds(0, chips)], sent(br, "hop"))

                drain(br.sums, sent(br, "sums"))

            @pl.when(section > wide_count)
            def _():
                drain(br.below, sent(br, "hop"))

        @pl.loop(0, count)
        def _(m):
            @pl.when(jnp.logical_and(helper(m) == section, owner(m) == me))
            def _():
                for br in branches:
                    drain(br.top.at[pl.ds(0, parts - 1), 0], br.top_sent.at[m // sections])

            @pl.when(jnp.logical_and(jnp.logical_not(is_last), helper(m) == section))
            def _():
                for br in branches:
                    drain(br.lifted.at[m // sections], br.lift_sent.at[m // sections])

        for br in branches:
            drain(br.columns_out, sent(br, "columns"))
            drain(br.local_out, sent(br, "local"))
            drain(br.below.at[pl.ds(0, count - size)], sent(br, "out"))
            drain(br.out.at[pl.ds(0, parts - 1)], br.out_got.at[0])


def branch_call(sections, scale, weights, saveds, tops):
    half, full = jnp.bfloat16, jnp.float32
    operands, outs, out_specs, scratch = [], [], [], []
    vmem = pl.BlockSpec(memory_space=pltpu.VMEM)
    anywhere = pl.BlockSpec(memory_space=pl.ANY)
    rows, width = weights[0].shape
    parts = width // rows
    size, tokens = saveds[0].shape[:2]
    volume = sum(saved.size * saved.dtype.itemsize for saved in saveds)
    roomy = parts == size and volume * parts <= 8 * 1024 * 1024
    chips = parts // 2
    count = size * parts
    kept = 1 if roomy else parts
    turns = -(-count // sections)
    for weight, saved, top in zip(weights, saveds, tops):
        rows = weight.shape[0]
        wide = -(-rows // 128) * 128
        main, rest = layout(rows, tokens)
        block = (tokens + tokens * rest // main, main)
        operands += [weight, saved, top]
        all_sums = (parts, rows, rows) if roomy else (1, 8, 128)
        outs += [
            jax.ShapeDtypeStruct((parts, size, *block), half),
            jax.ShapeDtypeStruct((kept, size, tokens, wide), half),
            jax.ShapeDtypeStruct((kept * size, parts, *block), half),
            jax.ShapeDtypeStruct(all_sums, full),
        ]
        out_specs += [vmem, anywhere, anywhere, anywhere]
        dma = pltpu.SemaphoreType.DMA
        slots = parts if roomy else 1
        scratch += [
            pltpu.VMEM((parts, size, tokens, wide), half),
            pltpu.VMEM((parts, size, *block), half),
            pltpu.VMEM((turns, *block), half),
            pltpu.VMEM((parts, size, tokens, wide), half),
            pltpu.VMEM((count, parts, *block), half),
            pltpu.VMEM((parts, wide, wide), half),
            pltpu.VMEM((parts * (main + rest), wide), half),
            pltpu.VMEM((count, slots, *block), half),
            pltpu.VMEM((count, *block), half),
            pltpu.VMEM((count, chips, *block), half),
            pltpu.VMEM((count, chips, *block), half),
            pltpu.VMEM((count, chips, *block), half),
            pltpu.VMEM((count, max(chips - 1, 1), *block), half),
            pltpu.VMEM((count, slots, *block), half),
            pltpu.VMEM(all_sums, full),
            dma((parts + 1,)),
            dma((count,)),
            dma((count,)),
            dma((count,)),
            dma((count,)),
            dma((count,)),
            dma((count if roomy else 1,)),
            dma((1,)),
            dma((len(SENDS),)),
            dma((turns,)),
            dma((turns,)),
            dma((turns,)),
            pltpu.VMEM(weight.shape, half),
            pltpu.VMEM(top.shape, half),
            dma((2,)),
        ]
    return roomy, pl.pallas_call(
        functools.partial(kernel, sections, parts, size, roomy, scale),
        out_shape=outs,
        in_specs=[anywhere, vmem, anywhere] * 2,
        out_specs=out_specs,
        scratch_shapes=scratch,
        compiler_params=pltpu.CompilerParams(
            collective_id=0, has_side_effects=True, vmem_limit_bytes=63 * 1024 * 1024
        ),
    )(*operands)


def finish_kernel(roomy, scale, *refs):
    outs, buffers, sems = refs[8:12], refs[12:16], refs[16]
    staged, in_sems = refs[17:25], refs[25]
    pending = []

    def load(i, *at):
        src, dst = (refs[i].at[at], staged[i].at[at]) if at else (refs[i], staged[i])
        return pltpu.make_async_copy(src, dst, in_sems.at[(i, *(at or (0,)))])

    def flush(src, dst):
        copy = pltpu.make_async_copy(src, dst, sems.at[len(pending)])
        copy.start()
        pending.append(copy)

    parts = staged[0].shape[0]
    for b in (1, 0):
        load(4 * b + 1).start()
        load(4 * b + 2).start()
        if roomy:
            for part in range(parts):
                load(4 * b + 3, part).start()
        load(4 * b).start()

    for b in (1, 0):
        grads_in, columns, local, sums_in = staged[4 * b : 4 * b + 4]
        grads, sums = outs[2 * b : 2 * b + 2]
        grad_buffer, sum_buffer = buffers[2 * b : 2 * b + 2]
        size, tokens = grad_buffer.shape[:2]
        wide = columns.shape[-1]
        rows = sum_buffer.shape[0]
        rest = layout(rows, tokens)[1]

        def whole(block):
            return jnp.concatenate(unfold(block, rest), axis=-1)[:, :rows]

        load(4 * b + 1).wait()
        load(4 * b + 2).wait()
        spans = [range(turn * size, (turn + 1) * size) for turn in range(columns.shape[0])]
        lefts = [columns[turn].reshape(size * tokens, wide)[:, :rows] for turn in range(columns.shape[0])]
        for part in range(parts):
            total = None
            for left, span in zip(lefts, spans):
                right = jnp.concatenate([whole(local[i, part]) for i in span], axis=0)
                term = lax.dot_general(
                    left, right, (((0,), (0,)), ((), ())), preferred_element_type=jnp.float32,
                )
                term = (term * scale).astype(jnp.bfloat16).astype(jnp.float32)
                total = term if total is None else total + term
            if roomy:
                load(4 * b + 3, part).wait()
                total = sums_in[part] + total
            sum_buffer[:, part * rows : (part + 1) * rows] = total
            if rows % 128 == 0:
                span = pl.ds(part * rows, rows)
                flush(sum_buffer.at[:, span], sums.at[:, span])
        if rows % 128:
            flush(sum_buffer, sums)
        load(4 * b).wait()
        for part in range(parts):
            for at in range(size):
                grad_buffer[at, :, part * rows : (part + 1) * rows] = whole(grads_in[part, at])
        flush(grad_buffer, grads)
    for copy in pending:
        copy.wait()


def finish(roomy, results, sizes, rows_of, scale):
    outs, buffers = [], []
    for b in range(2):
        parts = results[4 * b].shape[0]
        size, tokens = sizes
        rows = rows_of[b]
        shapes = [((size, tokens, parts * rows), jnp.bfloat16), ((rows, parts * rows), jnp.float32)]
        outs += [jax.ShapeDtypeStruct(*shape) for shape in shapes]
        buffers += [pltpu.VMEM(*shape) for shape in shapes]
    return pl.pallas_call(
        functools.partial(finish_kernel, roomy, scale),
        out_shape=outs,
        in_specs=[pl.BlockSpec(memory_space=pl.ANY)] * 8,
        out_specs=[pl.BlockSpec(memory_space=pl.ANY)] * 4,
        scratch_shapes=buffers
        + [pltpu.SemaphoreType.DMA((2 * parts + 4,))]
        + [pltpu.VMEM(result.shape, result.dtype) for result in results]
        + [pltpu.SemaphoreType.DMA((8, parts))],
        compiler_params=pltpu.CompilerParams(vmem_limit_bytes=63 * 1024 * 1024),
    )(*results)


def shards(vit_weight, t5_weight, vit_saved, t5_saved, vit_top_grad, t5_top_grad):
    sections = lax.axis_size("section")
    size, tokens = t5_top_grad.shape[:2]
    scale = 1.0 / (size * tokens)
    roomy, results = branch_call(
        sections,
        scale,
        [t5_weight[0], vit_weight[0]],
        [t5_saved[0], vit_saved[0]],
        [t5_top_grad, vit_top_grad],
    )
    t5_grads, t5_sum, vit_grads, vit_sum = finish(
        roomy, results, (size, tokens), [t5_weight.shape[1], vit_weight.shape[1]], scale
    )
    return vit_grads[None], t5_grads[None], vit_sum[None], t5_sum[None]


def solution(mesh):
    placed = (
        P("section", "dp", None),
        P("section", "dp", None),
        P("section", None, "dp", None),
        P("section", None, "dp", None),
        P(None, "dp", None),
        P(None, "dp", None),
    )
    return jax.shard_map(
        shards,
        mesh=mesh,
        in_specs=placed,
        out_specs=(
            P("section", None, "dp", None),
            P("section", None, "dp", None),
            P("section", "dp", None),
            P("section", "dp", None),
        ),
        check_vma=False,
    )
```

```python
import functools

import jax
import jax.numpy as jnp
from jax import lax
from jax.experimental import pallas as pl
from jax.experimental.pallas import tpu as pltpu
from jax.sharding import PartitionSpec as P

root_half = 0.7071067811865476
inv_root_tau = 0.3989422804014327
MESH = pl.DeviceIdType.MESH


def gelu_slope(preact):
    cumulative = 0.5 * (1.0 + lax.erf(preact * root_half))
    density = jnp.exp(-0.5 * preact * preact) * inv_root_tau
    return cumulative + preact * density


NAMES = (
    "saved", "top", "lifted", "columns", "local", "weight", "flip", "above", "below", "mine",
    "pair_out", "pair_in", "chip_in", "slopes", "sums", "saved_got", "above_got", "pair_got",
    "chip_got", "near_got", "far_got", "slope_got", "out_got", "sent", "top_sent", "top_got",
    "lift_sent",
    "weight_raw", "top_raw", "raw_got",
)
SENDS = ("saved", "pair", "chip", "near", "far", "slope", "hop", "out", "columns", "local", "sums")


class Branch:
    def __init__(self, ins, outs, scratch):
        self.weight_in, self.saved_in, self.top_in = ins
        self.out, self.columns_out, self.local_out, self.sums_out = outs
        for name, ref in zip(NAMES, scratch):
            setattr(self, name, ref)
        self.rows = self.weight_in.shape[0]
        self.tokens = self.saved_in.shape[1]
        self.main, self.rest = layout(self.rows, self.tokens)


def layout(rows, tokens):
    main = rows // 128 * 128
    rest = rows - main
    if rest and main and main % rest == 0 and tokens % (8 * (main // rest)) == 0:
        return main, rest
    return -(-rows // 128) * 128, 0


def fold(block, rest):
    if rest == 0:
        return block
    main = block.shape[1] - rest
    step = block.shape[0] * rest // main
    pieces = [block[first : first + step, main:] for first in range(0, block.shape[0], step)]
    return jnp.concatenate([block[:, :main], jnp.concatenate(pieces, axis=1)], axis=0)


def unfold(block, rest):
    if rest == 0:
        return [block]
    main = block.shape[1]
    tokens = block.shape[0] * main // (main + rest)
    tail = block[tokens:].astype(jnp.float32)
    pieces = [tail[:, first : first + rest] for first in range(0, main, rest)]
    return [block[:tokens], jnp.concatenate(pieces, axis=0).astype(block.dtype)]


def drain(ref, sem):
    pltpu.make_async_copy(ref, ref, sem).wait()


def kernel(sections, parts, size, roomy, scale, *refs):
    ins, outs, scratch = refs[:6], refs[6:14], refs[14:]
    branches = [
        Branch(ins[3 * b : 3 * b + 3], outs[4 * b : 4 * b + 4],
               scratch[len(NAMES) * b : len(NAMES) * (b + 1)])
        for b in range(2)
    ]
    count = size * parts
    first_size = size // 2 if size % 2 == 0 else size
    section = lax.axis_index("section")
    me = lax.axis_index("dp")
    chips = parts // 2
    chip, core = me // 2, me % 2
    partner = chip * 2 + 1 - core
    last = sections - 1
    is_last = section == last
    is_first = section == 0
    wide_count = sections // 2 + 1 if roomy else 0
    wide_flag = lax.min(lax.max(wide_count - section, 0), 1)
    wide_in = section < wide_count
    wide_out = jnp.logical_and(section > 0, section <= wide_count)
    lag = lax.min(1 + (1 - 1) * lax.max(section - last + 1, 0), count)
    narrow_sums = lax.min(3 + 4 * (last - section) * (last - section), count)
    first_sums = narrow_sums + (min(4, count) - narrow_sums) * wide_flag

    def slot(part):
        return part if roomy else 0

    def ahead(k):
        return lax.rem(chip + k, chips) * 2 + core

    def behind(k):
        return lax.rem(chip + chips - k, chips) * 2 + core

    def other(group):
        return group + 1 - 2 * core

    def owner(m):
        turn = m // size
        return lax.rem(turn, chips) * 2 + 1 - turn // chips

    def copy(src, dst, sent, got, where, part):
        return pltpu.make_async_remote_copy(
            src_ref=src, dst_ref=dst, send_sem=sent, recv_sem=got,
            device_id=(where, part), device_id_type=MESH,
        )

    def sent(br, name):
        return br.sent.at[SENDS.index(name)]

    def padded(block, wide):
        spare = wide - block.shape[-1]
        if spare:
            block = jnp.concatenate([block, jnp.zeros((*block.shape[:-1], spare), block.dtype)], axis=-1)
        return block

    def packed(br, block):
        return fold(block[:, : br.rows], br.rest) if br.rest else padded(block, br.main)

    def regroup(source, groups):
        cut = source.shape[-1] // parts
        for group in range(parts):
            groups[group] = padded(source[..., group * cut : (group + 1) * cut], groups.shape[-1])

    def weight_load(br):
        return pltpu.make_async_copy(br.weight_in, br.weight_raw, br.raw_got.at[0])

    def top_load(br):
        return pltpu.make_async_copy(br.top_in, br.top_raw, br.raw_got.at[1])

    for br in branches:
        top_load(br).start()
    for br in branches:
        weight_load(br).start()

    barrier = pltpu.get_barrier_semaphore()
    for k in range(1, parts):
        pl.semaphore_signal(barrier, inc=1, device_id=(section, lax.rem(me + k, parts)), device_id_type=MESH)

    def greet(other_section):
        for part in range(parts):
            pl.semaphore_signal(barrier, inc=1, device_id=(other_section, part), device_id_type=MESH)

    @pl.when(is_last)
    def _():
        @pl.loop(0, last)
        def _(lower):
            pl.semaphore_signal(barrier, inc=1, device_id=(lower, me), device_id_type=MESH)

    @pl.when(jnp.logical_not(is_last))
    def _():
        greet(section + 1)

    with jax.named_scope("regroup_saved"):
        for br in branches:
            regroup(br.saved_in, br.saved)
        for br in branches:
            top_load(br).wait()
            for group in range(parts):
                for at in range(size):
                    block = br.top_raw[at, :, group * br.rows : (group + 1) * br.rows]
                    br.top[group, at] = packed(br, block.astype(jnp.float32)).astype(jnp.bfloat16)
    greeted = parts * lax.min(section, 1) + lax.min(last - section, 1)
    with jax.named_scope("barrier"):
        pl.semaphore_wait(barrier, parts - 1 + greeted)

    def helper(m):
        return last - lax.rem(m, sections)

    def saved_copy(br, turn, k):
        to = lax.rem(me + k, parts)
        return copy(br.saved.at[to], br.columns.at[turn], sent(br, "saved"), br.saved_got.at[turn], section, to)

    def top_copy(br, m, k):
        to, turn = lax.rem(me + k, parts), m // sections
        return copy(br.top.at[to, lax.rem(m, size)], br.lifted.at[turn], br.top_sent.at[turn], br.top_got.at[turn], section, to)

    def lift_copy(br, m):
        turn = m // sections
        return copy(br.lifted.at[turn], br.above.at[m, slot(me)], br.lift_sent.at[turn], br.above_got.at[m], last, me)

    def batch(m):
        return lax.min(m, size + lax.max(m // size - 1, 0))

    def pair_copy(br, m):
        return copy(br.pair_out.at[m], br.pair_in.at[m], sent(br, "pair"), br.pair_got.at[batch(m)], section, partner)

    def chip_copy(br, m, k):
        return copy(br.mine.at[m, k], br.chip_in.at[m, k - 1], sent(br, "chip"), br.chip_got.at[m], section, ahead(k))

    def near_copy(br, m, k):
        group = behind(k)
        return copy(br.local.at[m, group], br.local.at[m, group], sent(br, "near"), br.near_got.at[m], section, partner)

    def far_copy(br, m, k):
        return copy(br.local.at[m, me], br.local.at[m, me], sent(br, "far"), br.far_got.at[m], section, ahead(k))

    def hop_copy(br, m, k):
        return copy(br.below.at[m], br.above.at[m, slot(me)], sent(br, "hop"), br.above_got.at[m], lax.max(section - 1, 0), ahead(k))

    def share_copy(br, m, k):
        group = behind(k)
        return copy(br.above.at[m, group], br.above.at[m, group], sent(br, "near"), br.near_got.at[m], section, partner)

    def slope_far(br, m, k):
        return copy(br.slopes.at[m, me], br.slopes.at[m, me], sent(br, "far"), br.far_got.at[m], section, ahead(k))

    def slope_near(br, m, k):
        group = behind(k)
        return copy(br.slopes.at[m, group], br.slopes.at[m, group], sent(br, "slope"), br.slope_got.at[m // size], section, partner)

    def out_copy(br, m):
        return copy(br.below.at[m], br.out.at[me, lax.rem(m, size)], sent(br, "out"), br.out_got.at[0], section, owner(m))

    def half_copy(br, h, k):
        to, span = lax.rem(me + k, parts), pl.ds(h * first_size, first_size)
        return copy(br.saved.at[to, span], br.columns.at[0, span], sent(br, "saved"), br.saved_got.at[h * parts], section, to)

    def piecewise(turn):
        return jnp.logical_and(is_last, turn >= chips)

    def piece_copy(br, m, k):
        to, turn, at = lax.rem(me + k, parts), m // size, lax.rem(m, size)
        return copy(br.saved.at[to, at], br.columns.at[turn, at], sent(br, "saved"), br.saved_got.at[turn], section, to)

    def send_piece(m):
        @pl.when(jnp.logical_and(piecewise(m // size), owner(m) == me))
        def _():
            for br in branches:
                for k in range(1, parts):
                    piece_copy(br, m, k).start()

    def send_saved(first, end):
        @pl.loop(first, end)
        def _(turn):
            @pl.when(owner(turn * size) == me)
            def _():
                for br in branches:
                    br.columns[turn] = br.saved[me]

                @pl.when(turn == 0)
                def _():
                    @pl.loop(0, size // first_size)
                    def _(h):
                        for br in branches:
                            for k in range(1, parts):
                                half_copy(br, h, k).start()

                @pl.when(turn > chips)
                def _():
                    pl.loop(0, first_size)(lambda at: send_piece(turn * size + at))

                @pl.when(jnp.logical_and(turn > 0, jnp.logical_not(piecewise(turn))))
                def _():
                    for br in branches:
                        for k in range(1, parts):
                            saved_copy(br, turn, k).start()

    def send_tops(first, end):
        @pl.loop(first, end)
        def _(m):
            @pl.when(jnp.logical_and(helper(m) == section, owner(m) == me))
            def _():
                for br in branches:
                    br.lifted[m // sections] = br.top[me, lax.rem(m, size)]
                    for k in range(1, parts):
                        top_copy(br, m, k).start()

    def wait_top(br, m):
        @pl.when(owner(m) != me)
        def _():
            drain(br.lifted.at[m // sections], br.top_got.at[m // sections])

    def lift(first, end):
        @pl.loop(first, end)
        def _(m):
            @pl.when(helper(m) == section)
            def _():
                for br in branches:
                    wait_top(br, m)
                    lift_copy(br, m).start()

    def partial_of(turn, at, length, got):
        first = turn * size + at

        @pl.when(owner(turn * size) != me)
        def _():
            for br in branches:
                drain(br.columns.at[turn, pl.ds(at, length)], br.saved_got.at[got])

        for br in branches:
            wide = br.columns.shape[-1]
            tokens = br.columns[turn, pl.ds(at, length)].reshape(-1, wide)

            def product(into, k, group):
                block = jnp.dot(tokens, br.weight[group], preferred_element_type=jnp.float32)
                for i in range(length):
                    piece = packed(br, block[i * br.tokens : (i + 1) * br.tokens])
                    into[first + i, k] = piece.astype(jnp.bfloat16)

            for k in range(chips):
                product(br.pair_out, k, other(ahead(k)))

            @pl.loop(first, first + length)
            def _(m):
                pair_copy(br, m).start()

            for k in range(chips):
                product(br.mine, k, ahead(k))

    @jax.named_scope("partial")
    def partial(turn):
        partial_of(turn, 0, size, turn)

    def pair_sum(m):
        for br in branches:
            @pl.when(m < size)
            def _():
                drain(br.pair_in.at[m], br.pair_got.at[batch(m)])

            @pl.when(jnp.logical_and(m >= size, lax.rem(m, size) == 0))
            def _():
                drain(br.pair_in.at[pl.ds(0, size)], br.pair_got.at[batch(m)])

            for k in range(1, chips):
                both = br.mine[m, k].astype(jnp.float32) + br.pair_in[m, k].astype(jnp.float32)
                br.mine[m, k] = both.astype(jnp.bfloat16)
                chip_copy(br, m, k).start()

    def find_slope(br, m):
        total = br.mine[m, 0].astype(jnp.float32) + br.pair_in[m, 0].astype(jnp.float32)
        if chips > 1:
            drain(br.chip_in.at[m], br.chip_got.at[m])
        for k in range(1, chips):
            total = total + br.chip_in[m, k - 1].astype(jnp.float32)
        br.slopes[m, slot(me)] = gelu_slope(total).astype(jnp.bfloat16)

    @jax.named_scope("spread")
    def spread(m):
        at_hand = jnp.logical_and(is_last, helper(m) == section)
        for br in branches:
            find_slope(br, m)

            @pl.when(at_hand)
            def _():
                wait_top(br, m)
                br.above[m, slot(me)] = br.lifted[m // sections]

            @pl.when(jnp.logical_not(at_hand))
            def _():
                drain(br.below.at[m], br.above_got.at[m])

            upper = br.above[m, slot(me)].astype(jnp.float32)
            br.local[m, me] = (upper * br.slopes[m, slot(me)].astype(jnp.float32)).astype(jnp.bfloat16)
            for k in range(1, chips):
                far_copy(br, m, k).start()
            near_copy(br, m, 0).start()

    @jax.named_scope("relay")
    def relay(m):
        for br in branches:
            if chips > 1:
                drain(br.local.at[m, pl.ds(0, chips - 1)], br.far_got.at[m])
            for k in range(1, chips):
                near_copy(br, m, k).start()

    def through(br, m, blocks):
        pieces = zip(*(unfold(block, br.rest) for block in blocks))
        blocks = [block for piece in pieces for block in piece]
        total = jnp.dot(jnp.concatenate(blocks, axis=-1), br.flip[...], preferred_element_type=jnp.float32)
        total = br.above[m, slot(me)].astype(jnp.float32) + packed(br, total)
        br.below[m] = total.astype(jnp.bfloat16)

        @pl.when(jnp.logical_not(is_first))
        def _():
            hop_copy(br, m, 0).start()

        @pl.when(wide_out)
        def _():
            for k in range(1, chips):
                hop_copy(br, m, k).start()

    @jax.named_scope("descend")
    def descend(m):
        for br in branches:
            drain(br.local.at[m, pl.ds(0, chips)], br.near_got.at[m])
            through(br, m, [br.local[m, group] for group in range(parts)])

    @jax.named_scope("share")
    def share(m):
        for br in branches:
            drain(br.local.at[m, pl.ds(0, chips)], br.above_got.at[m])
            for k in range(chips):
                share_copy(br, m, k).start()

    @jax.named_scope("descend_wide")
    def descend_wide(m):
        for br in branches:
            @pl.when(lax.rem(m, size) == 0)
            def _():
                drain(br.local.at[pl.ds(0, size), pl.ds(0, chips)], br.slope_got.at[m // size])

            drain(br.local.at[m, pl.ds(0, chips)], br.near_got.at[m])
            blocks = []
            for group in range(parts):
                block = br.above[m, group].astype(jnp.float32) * br.slopes[m, group].astype(jnp.float32)
                blocks.append(block.astype(jnp.bfloat16))
                br.local[m, group] = blocks[-1]
            through(br, m, blocks)

    def hand_out(m):
        for br in branches:
            @pl.when(owner(m) == me)
            def _():
                br.out[me, lax.rem(m, size)] = br.below[m]

            @pl.when(owner(m) != me)
            def _():
                out_copy(br, m).start()

    @jax.named_scope("sums")
    def add_sums(m):
        if not roomy:
            return
        turn, group = m // size - 1, lax.rem(m, size)

        @pl.when(turn >= 0)
        def _():
            for br in branches:
                wide = br.columns.shape[-1]
                left = br.columns[lax.max(turn, 0)].reshape(-1, wide)
                turn_start = lax.max(turn, 0) * size
                right = jnp.concatenate(
                    [jnp.concatenate(unfold(br.local[turn_start + i, group], br.rest), axis=-1) for i in range(size)],
                    axis=0,
                )
                left, right = left[:, : br.rows], right[:, : br.rows]
                term = lax.dot_general(left, right, (((0,), (0,)), ((), ())), preferred_element_type=jnp.float32)
                total = br.sums[group] + (term * scale).astype(jnp.bfloat16).astype(jnp.float32)
                br.sums[group] = total

                @pl.when(turn == parts - 2)
                def _():
                    pltpu.make_async_copy(br.sums.at[group], br.sums_out.at[group], sent(br, "sums")).start()

    early = min(sections, count)

    @pl.when(jnp.logical_not(is_last))
    def _():
        send_tops(0, early)

    send_saved(0, parts)

    @pl.when(is_last)
    def _():
        send_tops(0, early)

    send_tops(early, count)

    with jax.named_scope("regroup_weight"):
        for br in branches:
            rows = br.weight_in.shape[0]
            wide = br.weight.shape[-1]
            weight_load(br).wait()
            for group in range(parts):
                block = padded(br.weight_raw[:, group * rows : (group + 1) * rows], wide)
                br.weight[group, :rows] = block
                if wide > rows:
                    br.weight[group, rows:] = jnp.zeros((wide - rows, wide), block.dtype)

    with jax.named_scope("flip_weight"):
        for br in branches:
            wide = br.weight.shape[-1]

            @pl.loop(0, parts)
            def _(group):
                turned = br.weight[group].T
                br.flip[pl.ds(pl.multiple_of(group * br.main, 128), br.main), :] = turned[: br.main]
                if br.rest:
                    at = pl.multiple_of(parts * br.main + group * br.rest, br.rest)
                    br.flip[pl.ds(at, br.rest), :] = turned[br.main : br.rows]
                if roomy:
                    br.sums[group] = jnp.zeros(br.sums.shape[1:], jnp.float32)

    @pl.when(jnp.logical_not(is_last))
    def _():
        lift(0, early)

    @pl.loop(0, size // first_size)
    def _(h):
        with jax.named_scope("first_partial"):
            partial_of(0, h * first_size, first_size, h * parts)
        pl.loop(h * first_size, lax.min(first_sums, (h + 1) * first_size))(pair_sum)

    @pl.loop(0, max(size - 1, 1))
    def _(at):
        send_piece(at + chips * size)

    @pl.loop(chips + 1, parts)
    def _(turn):
        pl.loop(first_size, size)(lambda at: send_piece(turn * size + at))

    @pl.when(jnp.logical_not(is_last))
    def _():
        lift(early, count)
        pl.loop(1, parts)(partial)
        pl.loop(size, lax.max(first_sums, size))(pair_sum)

    def mixed(i):
        pair, at = i // (2 * size), lax.rem(i, 2 * size)
        return pair * 2 * size + lax.rem(at, 2) * size + at // 2

    def run_narrow():
        @pl.loop(0, count + lag + 1)
        def _(step):
            @pl.when(step < count)
            def _():
                spread(step)

            @pl.when(step < count - first_sums)
            def _():
                pair_sum(step + first_sums)

            @pl.when(step < size - max(size - 1, 1))
            def _():
                send_piece(chips * size + max(size - 1, 1) + step)

            @pl.when(jnp.logical_and(is_last, jnp.logical_and(step < count - size, lax.rem(step, size) == 0)))
            def _():
                partial(step // size + 1)

            @pl.when(jnp.logical_and(step > lag, step < count + lag + 1))
            def _():
                descend(step - lag - 1)

            @pl.when(jnp.logical_and(step >= lag, step < count + lag))
            def _():
                relay(step - lag)

            @pl.when(step > lag)
            def _():
                add_sums(step - lag - 1)

        pl.loop(0, count)(lambda i: hand_out(mixed(i)))

    def run_wide():
        def prepare(m):
            @pl.when(m < count)
            def _():
                for br in branches:
                    find_slope(br, m)
                    for k in range(1, chips):
                        slope_far(br, m, k).start()
                    slope_near(br, m, 0).start()

            @pl.when(m < count - first_sums)
            def _():
                pair_sum(m + first_sums)

            @pl.when(m >= 2)
            def _():
                for br in branches:
                    if chips > 1:
                        drain(br.local.at[m - 2, pl.ds(0, chips - 1)], br.far_got.at[m - 2])
                    for k in range(1, chips):
                        slope_near(br, m - 2, k).start()

        start = lax.min(10 + 2 * (wide_count - 1 - section), count + 2)
        with jax.named_scope("prepare"):
            pl.loop(0, start)(prepare)

        @pl.loop(0, count)
        def _(m):
            share(m)

            @pl.when(m > 0)
            def _():
                add_sums(lax.max(m - 1, 0))

            descend_wide(m)

            @pl.when(is_first)
            def _():
                hand_out(m)

            @pl.when(jnp.logical_and(section == 1, jnp.logical_and(m >= size, m < count - size)))
            def _():
                hand_out(mixed(lax.max(m - size, 0)))

            @pl.when(m + start < count + 2)
            def _():
                prepare(m + start)

        @pl.when(section == 1)
        def _():
            pl.loop(max(count - 2 * size, 0), count)(lambda i: hand_out(mixed(i)))

        @pl.when(section > 1)
        def _():
            pl.loop(0, count)(lambda i: hand_out(mixed(i)))

        add_sums(count - 1)

    if roomy:
        pl.when(jnp.logical_not(wide_in))(run_narrow)
        pl.when(wide_in)(run_wide)
    else:
        run_narrow()

    with jax.named_scope("final_waits"):
        for br in branches:
            kept = br.columns_out.shape[0]
            columns = br.columns.at[pl.ds(parts - kept, kept)]
            pltpu.make_async_copy(columns, br.columns_out, sent(br, "columns")).start()
            local = br.local.at[pl.ds(count - kept * size, kept * size)]
            pltpu.make_async_copy(local, br.local_out, sent(br, "local")).start()
        for br in branches:
            others = pl.ds(0, parts - 1)
            drain(br.saved.at[others], sent(br, "saved"))
            drain(br.pair_in, sent(br, "pair"))
            drain(br.local.at[:, pl.ds(0, chips)], sent(br, "near"))
            if chips > 1:
                drain(br.chip_in, sent(br, "chip"))
                drain(br.local.at[:, pl.ds(0, chips - 1)], sent(br, "far"))

            if roomy:
                @pl.when(wide_in)
                def _():
                    drain(br.local.at[:, pl.ds(0, chips)], sent(br, "slope"))

                @pl.when(wide_out)
                def _():
                    drain(br.local.at[:, pl.ds(0, chips)], sent(br, "hop"))

                drain(br.sums, sent(br, "sums"))

            @pl.when(section > wide_count)
            def _():
                drain(br.below, sent(br, "hop"))

        @pl.loop(0, count)
        def _(m):
            @pl.when(jnp.logical_and(helper(m) == section, owner(m) == me))
            def _():
                for br in branches:
                    drain(br.top.at[pl.ds(0, parts - 1), 0], br.top_sent.at[m // sections])

            @pl.when(jnp.logical_and(jnp.logical_not(is_last), helper(m) == section))
            def _():
                for br in branches:
                    drain(br.lifted.at[m // sections], br.lift_sent.at[m // sections])

        for br in branches:
            drain(br.columns_out, sent(br, "columns"))
            drain(br.local_out, sent(br, "local"))
            drain(br.below.at[pl.ds(0, count - size)], sent(br, "out"))
            drain(br.out.at[pl.ds(0, parts - 1)], br.out_got.at[0])


def branch_call(sections, scale, weights, saveds, tops):
    half, full = jnp.bfloat16, jnp.float32
    operands, outs, out_specs, scratch = [], [], [], []
    vmem = pl.BlockSpec(memory_space=pltpu.VMEM)
    anywhere = pl.BlockSpec(memory_space=pl.ANY)
    rows, width = weights[0].shape
    parts = width // rows
    size, tokens = saveds[0].shape[:2]
    volume = sum(saved.size * saved.dtype.itemsize for saved in saveds)
    roomy = parts == size and volume * parts <= 8 * 1024 * 1024
    chips = parts // 2
    count = size * parts
    kept = 1 if roomy else parts
    turns = -(-count // sections)
    for weight, saved, top in zip(weights, saveds, tops):
        rows = weight.shape[0]
        wide = -(-rows // 128) * 128
        main, rest = layout(rows, tokens)
        block = (tokens + tokens * rest // main, main)
        operands += [weight, saved, top]
        all_sums = (parts, rows, rows) if roomy else (1, 8, 128)
        outs += [
            jax.ShapeDtypeStruct((parts, size, *block), half),
            jax.ShapeDtypeStruct((kept, size, tokens, wide), half),
            jax.ShapeDtypeStruct((kept * size, parts, *block), half),
            jax.ShapeDtypeStruct(all_sums, full),
        ]
        out_specs += [vmem, anywhere, anywhere, anywhere]
        dma = pltpu.SemaphoreType.DMA
        slots = parts if roomy else 1
        scratch += [
            pltpu.VMEM((parts, size, tokens, wide), half),
            pltpu.VMEM((parts, size, *block), half),
            pltpu.VMEM((turns, *block), half),
            pltpu.VMEM((parts, size, tokens, wide), half),
            pltpu.VMEM((count, parts, *block), half),
            pltpu.VMEM((parts, wide, wide), half),
            pltpu.VMEM((parts * (main + rest), wide), half),
            pltpu.VMEM((count, slots, *block), half),
            pltpu.VMEM((count, *block), half),
            pltpu.VMEM((count, chips, *block), half),
            pltpu.VMEM((count, chips, *block), half),
            pltpu.VMEM((count, chips, *block), half),
            pltpu.VMEM((count, max(chips - 1, 1), *block), half),
            pltpu.VMEM((count, slots, *block), half),
            pltpu.VMEM(all_sums, full),
            dma((parts + 1,)),
            dma((count,)),
            dma((size + parts,)),
            dma((count,)),
            dma((count,)),
            dma((count,)),
            dma((parts,)),
            dma((1,)),
            dma((len(SENDS),)),
            dma((turns,)),
            dma((turns,)),
            dma((turns,)),
            pltpu.VMEM(weight.shape, half),
            pltpu.VMEM(top.shape, half),
            dma((2,)),
        ]
    return roomy, pl.pallas_call(
        functools.partial(kernel, sections, parts, size, roomy, scale),
        out_shape=outs,
        in_specs=[anywhere, vmem, anywhere] * 2,
        out_specs=out_specs,
        scratch_shapes=scratch,
        compiler_params=pltpu.CompilerParams(
            collective_id=0, has_side_effects=True, vmem_limit_bytes=63 * 1024 * 1024
        ),
    )(*operands)


def finish_kernel(roomy, scale, *refs):
    outs, buffers, sems = refs[8:12], refs[12:16], refs[16]
    staged, in_sems = refs[17:25], refs[25]
    pending = []

    def load(i, *at):
        src, dst = (refs[i].at[at], staged[i].at[at]) if at else (refs[i], staged[i])
        return pltpu.make_async_copy(src, dst, in_sems.at[(i, *(at or (0,)))])

    def flush(src, dst):
        copy = pltpu.make_async_copy(src, dst, sems.at[len(pending)])
        copy.start()
        pending.append(copy)

    parts = staged[0].shape[0]
    for b in (1, 0):
        load(4 * b + 1).start()
        load(4 * b + 2).start()
        if roomy:
            for part in range(parts):
                load(4 * b + 3, part).start()
        load(4 * b).start()

    for b in (1, 0):
        grads_in, columns, local, sums_in = staged[4 * b : 4 * b + 4]
        grads, sums = outs[2 * b : 2 * b + 2]
        grad_buffer, sum_buffer = buffers[2 * b : 2 * b + 2]
        size, tokens = grad_buffer.shape[:2]
        wide = columns.shape[-1]
        rows = sum_buffer.shape[0]
        rest = layout(rows, tokens)[1]

        def whole(block):
            return jnp.concatenate(unfold(block, rest), axis=-1)[:, :rows]

        load(4 * b + 1).wait()
        load(4 * b + 2).wait()
        spans = [range(turn * size, (turn + 1) * size) for turn in range(columns.shape[0])]
        lefts = [columns[turn].reshape(size * tokens, wide)[:, :rows] for turn in range(columns.shape[0])]
        for part in range(parts):
            total = None
            for left, span in zip(lefts, spans):
                right = jnp.concatenate([whole(local[i, part]) for i in span], axis=0)
                term = lax.dot_general(
                    left, right, (((0,), (0,)), ((), ())), preferred_element_type=jnp.float32,
                )
                term = (term * scale).astype(jnp.bfloat16).astype(jnp.float32)
                total = term if total is None else total + term
            if roomy:
                load(4 * b + 3, part).wait()
                total = sums_in[part] + total
            sum_buffer[:, part * rows : (part + 1) * rows] = total
            if rows % 128 == 0:
                span = pl.ds(part * rows, rows)
                flush(sum_buffer.at[:, span], sums.at[:, span])
        if rows % 128:
            flush(sum_buffer, sums)
        load(4 * b).wait()
        for part in range(parts):
            for at in range(size):
                grad_buffer[at, :, part * rows : (part + 1) * rows] = whole(grads_in[part, at])
        flush(grad_buffer, grads)
    for copy in pending:
        copy.wait()


def finish(roomy, results, sizes, rows_of, scale):
    outs, buffers = [], []
    for b in range(2):
        parts = results[4 * b].shape[0]
        size, tokens = sizes
        rows = rows_of[b]
        shapes = [((size, tokens, parts * rows), jnp.bfloat16), ((rows, parts * rows), jnp.float32)]
        outs += [jax.ShapeDtypeStruct(*shape) for shape in shapes]
        buffers += [pltpu.VMEM(*shape) for shape in shapes]
    return pl.pallas_call(
        functools.partial(finish_kernel, roomy, scale),
        out_shape=outs,
        in_specs=[pl.BlockSpec(memory_space=pl.ANY)] * 8,
        out_specs=[pl.BlockSpec(memory_space=pl.ANY)] * 4,
        scratch_shapes=buffers
        + [pltpu.SemaphoreType.DMA((2 * parts + 4,))]
        + [pltpu.VMEM(result.shape, result.dtype) for result in results]
        + [pltpu.SemaphoreType.DMA((8, parts))],
        compiler_params=pltpu.CompilerParams(vmem_limit_bytes=63 * 1024 * 1024),
    )(*results)


def shards(vit_weight, t5_weight, vit_saved, t5_saved, vit_top_grad, t5_top_grad):
    sections = lax.axis_size("section")
    size, tokens = t5_top_grad.shape[:2]
    scale = 1.0 / (size * tokens)
    roomy, results = branch_call(
        sections,
        scale,
        [t5_weight[0], vit_weight[0]],
        [t5_saved[0], vit_saved[0]],
        [t5_top_grad, vit_top_grad],
    )
    t5_grads, t5_sum, vit_grads, vit_sum = finish(
        roomy, results, (size, tokens), [t5_weight.shape[1], vit_weight.shape[1]], scale
    )
    return vit_grads[None], t5_grads[None], vit_sum[None], t5_sum[None]


def solution(mesh):
    placed = (
        P("section", "dp", None),
        P("section", "dp", None),
        P("section", None, "dp", None),
        P("section", None, "dp", None),
        P(None, "dp", None),
        P(None, "dp", None),
    )
    return jax.shard_map(
        shards,
        mesh=mesh,
        in_specs=placed,
        out_specs=(
            P("section", None, "dp", None),
            P("section", None, "dp", None),
            P("section", "dp", None),
            P("section", "dp", None),
        ),
        check_vma=False,
    )
```
